512 devices in a mesh: row: 16 (over y_lo, z), col: 8 (over x, core), dp: 4 (over y_hi).
Axes of the slice: x: 4, y: 8 (y_hi: 4, y_lo: 2; y = y_hi * 2 + y_lo), z: 8, core: 2. Of those that a mesh axis runs over, the one named last changes fastest.
Arguments:
- tokens: bfloat16 [1536, 6144], P('dp', 'row'), parts along dimension 0, may hold values from -120 to 120
- norm_gain: float32 [6144], P('row'), may hold values from 0.25 to 1.75
- qkv_weight: bfloat16 [6144, 3, 3072], P('row', None, 'col'), may hold values from -2.5 to 2.5
- out_weight: bfloat16 [3072, 6144], P('col', 'row'), may hold values from -0.109375 to 0.109375
Outputs:
- projected: bfloat16 [1536, 6144], P('dp', 'row'), parts along dimension 0
The draws below stay inside these ranges and needn't reach their ends.
There are 4 independent parts, one for each index of `dp`. The reference program is written for one: setup_inputs(seed, part) draws one part's arguments, and reference() takes and returns one part's arrays. A program takes and returns all parts, laid end to end along the dimension named above; an argument that names none is the same for every part. Nothing has to cross between parts.
All inputs are finite; a program needn't handle non-finite values.
Results may differ from the reference program's by a relative error of at most 0.025.
Values may be sent and summed in bfloat16 or wider, within the bound.
No kernel may reach another device: no remote copies, remote signals or barrier semaphores. Data moves between devices by JAX's collectives and lax.ppermute only.
A program may use at most 64 MiB of HBM per device.

```python
import math
import jax
import jax.numpy as jnp
from jax import lax

D = 6144
H = 24
K = 128
SEQ = 384
N_ROW = 16


def draw_tokens(key, part):
    subkeys = jax.random.split(key, 4)
    position = jnp.arange(D, dtype=jnp.float32) / D
    texture = jnp.exp(jax.random.uniform(subkeys[0], (1, D), jnp.float32, jnp.log(0.7), jnp.log(1.4)))
    row_scale = jnp.exp(jax.random.uniform(subkeys[1], (SEQ, 1), jnp.float32, jnp.log(0.5), jnp.log(2.0)))
    offset = jnp.clip(jax.random.normal(subkeys[2], (SEQ, 1), jnp.float32), -3.0, 3.0)
    feature_ramp = 10.0 ** (position - 0.5)
    jitter = jnp.clip(jax.random.normal(subkeys[3], (SEQ, D), jnp.float32), -4.0, 4.0)
    values = row_scale * feature_ramp * (offset + jitter * texture)
    return jnp.clip(values, -120.0, 120.0).astype(jnp.bfloat16)


def draw_qkv_weight(key, part):
    subkeys = jax.random.split(key, 1)
    weights = jnp.clip(jax.random.normal(subkeys[0], (D, 3, H * K), jnp.float32), -6.0, 6.0) / math.sqrt(D)
    return jnp.clip(weights, -2.5, 2.5).astype(jnp.bfloat16)


def block_scale(own_key, dims, cuts, low, top_value):
    level = 1.0
    for axis_at, blocks in cuts:
        heights = jax.random.uniform(jax.random.fold_in(jax.random.fold_in(own_key, 6), axis_at), (blocks,), jnp.float32, low / len(cuts), top_value / len(cuts))
        level = level * jnp.repeat(jnp.exp(heights), dims[axis_at] // blocks).reshape((-1,) + (1,) * (len(dims) - 1 - axis_at))
    return level


def bell_draw(stream_key, dims, deviation, reach, shards=(), kind=jnp.bfloat16):
    level = block_scale(stream_key, dims, shards, -0.22, 0.18) if shards else 1.0
    entries = jax.random.normal(stream_key, dims, jnp.float32) * deviation * level
    return jnp.minimum(jnp.maximum(entries, -reach), reach).astype(kind)


def setup_inputs(seed: int = 0, part: int = 0) -> dict:
    key_of = jax.random.split(jax.random.key(seed), 5)
    part_splits = jax.random.split(jax.random.fold_in(key_of[4], part), 5)
    return {
        "tokens": draw_tokens(jax.random.fold_in(jax.random.fold_in(key_of[4], part), 71), part),
        "norm_gain": jnp.clip(1.0 + 0.15 * jax.random.normal(key_of[1], (D,), jnp.float32), 0.25, 1.75),
        "qkv_weight": draw_qkv_weight(jax.random.fold_in(key_of[4], 71), part),
        "out_weight": bell_draw(key_of[3], (H * K, D), (H * K) ** -0.5, 0.109375, ((0, 8), (1, 16))),
    }


EPSILON = 1e-05

def normalize(tokens, norm_gain):
    values = tokens.astype(jnp.float32)
    average = lax.optimization_barrier(jnp.mean(values, axis=1, keepdims=True))
    centered = values - average
    variance = lax.optimization_barrier(jnp.mean(centered * centered, axis=1, keepdims=True))
    return (centered * lax.rsqrt(variance + EPSILON) * norm_gain).astype(jnp.bfloat16)

def project(normed, qkv_weight):
    block_width = D // N_ROW
    flattened = qkv_weight.reshape(D, 3 * H * K)
    totals = jnp.zeros((SEQ, 3 * H * K), jnp.float32)
    for row_block in range(N_ROW):
        first_feature = row_block * block_width
        partial_value = jnp.dot(normed[:, first_feature:first_feature + block_width], flattened[first_feature:first_feature + block_width], preferred_element_type=jnp.float32)
        rounded = lax.optimization_barrier(partial_value.astype(jnp.bfloat16))
        totals = totals + rounded.astype(jnp.float32)
    return totals.astype(jnp.bfloat16).reshape(SEQ, 3, H, K)

def attend_head(operands):
    query_part, key_part, value_part = operands
    scores = jnp.dot(query_part, key_part.T, preferred_element_type=jnp.float32) * (1.0 / math.sqrt(K))
    largest = lax.optimization_barrier(jnp.max(scores, axis=1, keepdims=True))
    exponent = jnp.exp(scores - largest)
    softmax_weights = (exponent / lax.optimization_barrier(jnp.sum(exponent, axis=1, keepdims=True))).astype(jnp.bfloat16)
    return jnp.dot(softmax_weights, value_part, preferred_element_type=jnp.float32).astype(jnp.bfloat16)

def reference(tokens, norm_gain, qkv_weight, out_weight):
    normed = normalize(tokens, norm_gain)
    stacked = jnp.transpose(project(normed, qkv_weight), (1, 2, 0, 3))
    attended = lax.map(attend_head, (stacked[0], stacked[1], stacked[2]))
    attended = jnp.transpose(attended, (1, 0, 2)).reshape(SEQ, H * K)
    return jnp.dot(attended, out_weight, preferred_element_type=jnp.float32).astype(jnp.bfloat16)
```

```python
import math

import jax
import jax.numpy as jnp
from jax import lax
from jax.experimental import pallas as pl
from jax.experimental.pallas import tpu as pltpu
from jax.sharding import PartitionSpec as P

K = 128
EPSILON = 1e-05
EXTRA = 128
HALF = 64
LIMIT = pltpu.CompilerParams(vmem_limit_bytes=20 * 2**20)


def rounded(a):
    return a.astype(jnp.bfloat16).astype(jnp.float32)


def dot32(a, b):
    return jnp.dot(a, b, preferred_element_type=jnp.float32)


def partial_kernel(devices, x_ref, g_ref, w_ref, o_ref):
    tokens, width = x_ref.shape
    columns = w_ref.shape[2]
    values = x_ref[...].astype(jnp.float32)
    middle = rounded(jnp.sum(values, axis=1, keepdims=True) / width)
    centered = values - middle
    total = jnp.sum(centered, axis=1, keepdims=True)
    square = jnp.sum(centered * centered, axis=1, keepdims=True)
    gain = g_ref[...]
    scaled = (centered * gain).astype(jnp.bfloat16)
    high = rounded(gain)
    line = lax.broadcasted_iota(jnp.int32, (16, width), 0)
    gains = jnp.where(line == 0, high, jnp.where(line == 1, gain - high, 0.0)).astype(jnp.bfloat16)
    per = tokens // devices
    row = lax.broadcasted_iota(jnp.int32, (per, EXTRA), 0)
    sums = jnp.zeros((per, EXTRA), jnp.float32)
    chunk = 0
    chunks = 3 * columns // EXTRA
    for part in range(3):
        weight = w_ref[part]
        o_ref[:, part * columns : (part + 1) * columns] = dot32(scaled, weight).astype(jnp.bfloat16)
        c = jnp.sum(dot32(gains, weight), axis=0, keepdims=True)
        for at in range(0, columns, EXTRA):
            piece = c[:, at : at + EXTRA]
            sums = jnp.where(row == chunk, piece, sums)
            sums = jnp.where(row == chunks + chunk, pltpu.roll(piece, HALF, 1), sums)
            chunk += 1
    lane = lax.broadcasted_iota(jnp.int32, (tokens, EXTRA), 1)
    extra = jnp.concatenate([sums] * devices, axis=0)
    for at, column in enumerate(
        (middle, rounded(total), total - rounded(total), rounded(square), square - rounded(square))
    ):
        extra = jnp.where(lane == at, column, extra)
    o_ref[:, 3 * columns :] = extra.astype(jnp.bfloat16)


def norm_kernel(width, r_ref, o_ref):
    devices, per, _ = r_ref.shape
    columns = o_ref.shape[1]
    chunks = columns // EXTRA
    extras = [r_ref[d, :, columns:].astype(jnp.float32) for d in range(devices)]
    middles = [e[:, 0:1] for e in extras]
    totals = [e[:, 1:2] + e[:, 2:3] for e in extras]
    squares = [e[:, 3:4] + e[:, 4:5] for e in extras]
    average = sum(m + t / width for m, t in zip(middles, totals)) / devices
    shifts = [m - average for m in middles]
    variance = sum(
        q + 2.0 * s * t + width * (s * s) for q, s, t in zip(squares, shifts, totals)
    ) / (width * devices)
    scale = lax.rsqrt(variance + EPSILON)
    wide = [jnp.broadcast_to(s, (per, EXTRA)) for s in shifts]
    turned = [pltpu.roll(e, HALF, 1) for e in extras]
    upper = lax.broadcasted_iota(jnp.int32, (1, EXTRA), 1) >= HALF
    for at in range(chunks):
        running = jnp.zeros((per, EXTRA), jnp.float32)
        for d in range(devices):
            c = jnp.where(
                upper, extras[d][at : at + 1], turned[d][chunks + at : chunks + at + 1]
            )
            term = r_ref[d, :, at * EXTRA : (at + 1) * EXTRA].astype(jnp.float32)
            running = running + term + wide[d] * c
        o_ref[:, at * EXTRA : (at + 1) * EXTRA] = (running * scale).astype(jnp.bfloat16)


def attend_kernel(x_ref, w_ref, o_ref):
    columns = w_ref.shape[0]
    scaling = 1.0 / math.sqrt(K)
    outs = []
    for at in range(0, columns, K):
        q = x_ref[:, at : at + K]
        k = x_ref[:, columns + at : columns + at + K]
        v = x_ref[:, 2 * columns + at : 2 * columns + at + K]
        scores = (
            lax.dot_general(q, k, (((1,), (1,)), ((), ())), preferred_element_type=jnp.float32)
            * scaling
        )
        largest = jnp.max(scores, axis=1, keepdims=True)
        exponent = jnp.exp(scores - largest)
        inverse = 1.0 / jnp.sum(exponent, axis=1, keepdims=True)
        outs.append(dot32((exponent * inverse).astype(jnp.bfloat16), v).astype(jnp.bfloat16))
    attended = jnp.concatenate(outs, axis=1)
    o_ref[...] = dot32(attended, w_ref[...]).astype(jnp.bfloat16)


def exchange(a, axis):
    return lax.all_to_all(a, axis, 0, 0, tiled=True)


def spread(a, axis):
    devices = lax.axis_size(axis)
    return exchange(jnp.broadcast_to(a[None], (devices, *a.shape)), axis)


def shards(tokens, norm_gain, qkv_weight, out_weight):
    count, width = tokens.shape
    columns = qkv_weight.shape[2]
    rows = lax.axis_size("row")
    cols = lax.axis_size("col")
    payload = pl.pallas_call(
        lambda *refs: partial_kernel(rows, *refs),
        out_shape=jax.ShapeDtypeStruct((count, 3 * columns + EXTRA), jnp.bfloat16),
        name="partial",
        compiler_params=LIMIT,
    )(tokens, norm_gain.reshape(1, width), jnp.transpose(qkv_weight, (1, 0, 2)))
    arrived = exchange(payload.reshape(rows, count // rows, 3 * columns + EXTRA), "row")
    own = pl.pallas_call(
        lambda *refs: norm_kernel(width, *refs),
        out_shape=jax.ShapeDtypeStruct((count // rows, 3 * columns), jnp.bfloat16),
        name="norm",
        compiler_params=LIMIT,
    )(arrived)
    qkv = spread(own, "row").reshape(count, 3 * columns)
    partial_out = pl.pallas_call(
        attend_kernel,
        out_shape=jax.ShapeDtypeStruct((count, width), jnp.bfloat16),
        name="attend",
        compiler_params=LIMIT,
    )(qkv, out_weight)
    terms = exchange(partial_out.reshape(cols, count // cols, width), "col")
    done = jnp.sum(terms.astype(jnp.float32), axis=0).astype(jnp.bfloat16)
    return spread(done, "col").reshape(count, width)


def solution(mesh):
    in_specs = (P("dp", "row"), P("row"), P("row", None, "col"), P("col", "row"))
    out_specs = P("dp", "row")
    return jax.shard_map(shards, mesh=mesh, in_specs=in_specs, out_specs=out_specs, check_vma=False)
```

```python
import math

import jax
import jax.numpy as jnp
from jax import lax
from jax.experimental import pallas as pl
from jax.experimental.pallas import tpu as pltpu
from jax.sharding import PartitionSpec as P

K = 128
EPSILON = 1e-05
EXTRA = 128
HALF = 64
LIMIT = pltpu.CompilerParams(vmem_limit_bytes=20 * 2**20)

RING = 8
CLASSES = 4
FORWARD = [(8 * y + z, 8 * y + (z + 1) % RING) for y in range(2) for z in range(RING)]
BACKWARD = [(8 * y + z, 8 * y + (z - 1) % RING) for y in range(2) for z in range(RING)]
ACROSS = [(r, (r + 8) % 16) for r in range(16)]
MEMBERS = [
    [8 * (j % 2) + (k - 2 * (j % 2) + 4 * (j // 2)) % RING for j in range(4)]
    for k in range(CLASSES)
]
CORES = [(c, c ^ 1) for c in range(8)]
CHIPS = [[0, 2, 4, 6], [1, 3, 5, 7]]


def rounded(a):
    return a.astype(jnp.bfloat16).astype(jnp.float32)


def dot32(a, b):
    return jnp.dot(a, b, preferred_element_type=jnp.float32)


def own_class():
    at = lax.axis_index("row")
    return lax.rem(at + 2 * lax.div(at, RING), CLASSES)


def block_start(step, size):
    return pl.multiple_of(lax.rem(own_class() + step, CLASSES) * size, size)


def with_statistics(base, columns):
    lane = lax.broadcasted_iota(jnp.int32, base.shape, 1)
    middle, total, square = columns
    for at, column in enumerate(
        (middle, rounded(total), total - rounded(total), rounded(square), square - rounded(square))
    ):
        base = jnp.where(lane == at, column, base)
    return base.astype(jnp.bfloat16)


def statistics(extra):
    return extra[:, 0:1], extra[:, 1:2] + extra[:, 2:3], extra[:, 3:4] + extra[:, 4:5]


def partial_kernel(per, x_ref, g_ref, w_ref, *o_refs):
    tokens, width = x_ref.shape
    columns = w_ref.shape[2]
    size = tokens // CLASSES
    values = jnp.concatenate(
        [x_ref[pl.ds(block_start(step, size), size), :] for step in range(CLASSES)], axis=0
    ).astype(jnp.float32)
    middle = rounded(jnp.sum(values, axis=1, keepdims=True) / width)
    centered = values - middle
    total = jnp.sum(centered, axis=1, keepdims=True)
    square = jnp.sum(centered * centered, axis=1, keepdims=True)
    gain = g_ref[...]
    scaled = (centered * gain).astype(jnp.bfloat16)
    high = rounded(gain)
    line = lax.broadcasted_iota(jnp.int32, (16, width), 0)
    gains = jnp.where(line == 0, high, jnp.where(line == 1, gain - high, 0.0)).astype(jnp.bfloat16)
    row = lax.broadcasted_iota(jnp.int32, (per, EXTRA), 0)
    sums = jnp.zeros((per, EXTRA), jnp.float32)
    chunk = 0
    chunks = 3 * columns // EXTRA
    for part in range(3):
        weight = w_ref[part]
        product = dot32(scaled, weight).astype(jnp.bfloat16)
        for step in range(CLASSES):
            o_refs[step][:, part * columns : (part + 1) * columns] = product[
                step * size : (step + 1) * size
            ]
        c = jnp.sum(dot32(gains, weight), axis=0, keepdims=True)
        for at in range(0, columns, EXTRA):
            piece = c[:, at : at + EXTRA]
            sums = jnp.where(row == chunk, piece, sums)
            sums = jnp.where(row == chunks + chunk, pltpu.roll(piece, HALF, 1), sums)
            chunk += 1
    base = jnp.concatenate([sums] * (tokens // per), axis=0)
    extra = with_statistics(base, (middle, total, square))
    for step in range(CLASSES):
        o_refs[step][:, 3 * columns :] = extra[step * size : (step + 1) * size]


def vector_sums(extras, chunks):
    upper = lax.broadcasted_iota(jnp.int32, (1, EXTRA), 1) >= HALF
    turned = [pltpu.roll(e, HALF, 1) for e in extras]
    return [
        [
            jnp.where(upper, e[at : at + 1], t[chunks + at : chunks + at + 1])
            for e, t in zip(extras, turned)
        ]
        for at in range(chunks)
    ]


def merge_kernel(per, width, *refs):
    terms, o_ref = refs[:-1], refs[-1]
    size = o_ref.shape[0]
    columns = o_ref.shape[1] - EXTRA
    chunks = columns // EXTRA
    extras = [t[:, columns:].astype(jnp.float32) for t in terms]
    held = [statistics(e) for e in extras]
    middle = rounded(sum(m + t / width for m, t, _ in held) / len(terms))
    shifts = [m - middle for m, _, _ in held]
    total = sum(t + width * s for s, (_, t, _) in zip(shifts, held))
    square = sum(q + 2.0 * s * t + width * (s * s) for s, (_, t, q) in zip(shifts, held))
    pieces = vector_sums([e[:per] for e in extras], chunks)
    wide = [jnp.broadcast_to(s, (size, EXTRA)) for s in shifts]
    for at in range(chunks):
        running = jnp.zeros((size, EXTRA), jnp.float32)
        for t, w, c in zip(terms, wide, pieces[at]):
            running = running + t[:, at * EXTRA : (at + 1) * EXTRA].astype(jnp.float32) + w * c
        o_ref[:, at * EXTRA : (at + 1) * EXTRA] = running.astype(jnp.bfloat16)
    lines = sum(e[:per] for e in extras)
    base = jnp.concatenate([lines] * (size // per), axis=0)
    o_ref[:, columns:] = with_statistics(base, (middle, total, square))


def norm_kernel(width, r_ref, o_ref):
    blocks, per, _ = r_ref.shape
    columns = o_ref.shape[1]
    chunks = columns // EXTRA
    extras = [r_ref[d, :, columns:].astype(jnp.float32) for d in range(blocks)]
    held = [statistics(e) for e in extras]
    average = sum(m + t / width for m, t, _ in held) / blocks
    shifts = [m - average for m, _, _ in held]
    variance = sum(
        q + 2.0 * s * t + width * (s * s) for s, (_, t, q) in zip(shifts, held)
    ) / (width * blocks)
    scale = lax.rsqrt(variance + EPSILON)
    wide = [jnp.broadcast_to(s, (per, EXTRA)) for s in shifts]
    pieces = vector_sums(extras, chunks)
    for at in range(chunks):
        running = jnp.zeros((per, EXTRA), jnp.float32)
        for d in range(blocks):
            term = r_ref[d, :, at * EXTRA : (at + 1) * EXTRA].astype(jnp.float32)
            running = running + term + wide[d] * pieces[at][d]
        o_ref[:, at * EXTRA : (at + 1) * EXTRA] = (running * scale).astype(jnp.bfloat16)


def attend_kernel(own_ref, one_ref, two_ref, three_ref, w_ref, keep_ref, send_ref, whole_ref):
    columns = w_ref.shape[0]
    scaling = 1.0 / math.sqrt(K)
    blocks = (own_ref, one_ref, two_ref, three_ref)
    size = own_ref.shape[0]

    def joined(at):
        return jnp.concatenate([b[:, at : at + K] for b in blocks], axis=0)

    outs = []
    for at in range(0, columns, K):
        q, k, v = joined(at), joined(columns + at), joined(2 * columns + at)
        scores = (
            lax.dot_general(q, k, (((1,), (1,)), ((), ())), preferred_element_type=jnp.float32)
            * scaling
        )
        largest = jnp.max(scores, axis=1, keepdims=True)
        exponent = jnp.exp(scores - largest)
        inverse = 1.0 / jnp.sum(exponent, axis=1, keepdims=True)
        outs.append(dot32((exponent * inverse).astype(jnp.bfloat16), v).astype(jnp.bfloat16))
    result = dot32(jnp.concatenate(outs, axis=1), w_ref[...]).astype(jnp.bfloat16)
    for step in range(CLASSES):
        whole_ref[pl.ds(block_start(step, size), size), :] = result[step * size : (step + 1) * size]
    half = keep_ref.shape[0]
    core = lax.rem(lax.axis_index("col"), 2)
    keep_ref[...] = whole_ref[pl.ds(pl.multiple_of(core * half, half), half), :]
    send_ref[...] = whole_ref[pl.ds(pl.multiple_of((1 - core) * half, half), half), :]


def exchange(a, axis, groups):
    return lax.all_to_all(a, axis, 0, 0, tiled=True, axis_index_groups=groups)


def spread(a, axis, groups):
    return exchange(jnp.broadcast_to(a[None], (len(groups[0]), *a.shape)), axis, groups)


def like(shape):
    return jax.ShapeDtypeStruct(shape, jnp.bfloat16)


def shards(tokens, norm_gain, qkv_weight, out_weight):
    count, width = tokens.shape
    columns = qkv_weight.shape[2]
    size = count // CLASSES
    per = size // len(MEMBERS[0])
    wide = 3 * columns + EXTRA
    own, ahead, over, behind = pl.pallas_call(
        lambda *refs: partial_kernel(per, *refs),
        out_shape=[like((size, wide))] * CLASSES,
        name="partial",
        compiler_params=LIMIT,
    )(tokens, norm_gain.reshape(1, width), jnp.transpose(qkv_weight, (1, 0, 2)))
    over = lax.ppermute(over, "row", ACROSS)
    ahead = lax.ppermute(ahead, "row", FORWARD)
    behind = lax.ppermute(behind, "row", BACKWARD)
    merged = pl.pallas_call(
        lambda *refs: merge_kernel(per, width, *refs),
        out_shape=like((size, wide)),
        name="merge",
        compiler_params=LIMIT,
    )(own, over, ahead, behind)
    arrived = exchange(merged.reshape(-1, per, wide), "row", MEMBERS)
    mine = pl.pallas_call(
        lambda *refs: norm_kernel(width * CLASSES, *refs),
        out_shape=like((per, 3 * columns)),
        name="norm",
        compiler_params=LIMIT,
    )(arrived)
    block = spread(mine, "row", MEMBERS).reshape(size, 3 * columns)
    second = lax.ppermute(block, "row", ACROSS)
    third = lax.ppermute(block, "row", FORWARD)
    first = lax.ppermute(block, "row", BACKWARD)
    keep, send = pl.pallas_call(
        attend_kernel,
        out_shape=[like((count // 2, width))] * 2,
        scratch_shapes=[pltpu.VMEM((count, width), jnp.bfloat16)],
        name="attend",
        compiler_params=LIMIT,
    )(block, first, second, third, out_weight)
    other = lax.ppermute(send, "col", CORES)
    pair = (keep.astype(jnp.float32) + other.astype(jnp.float32)).astype(jnp.bfloat16)
    terms = spread(pair, "col", CHIPS)
    half = jnp.sum(terms.astype(jnp.float32), axis=0).astype(jnp.bfloat16)
    rest = lax.ppermute(half, "col", CORES)
    core = lax.rem(lax.axis_index("col"), 2)
    return jnp.concatenate(
        [jnp.where(core == 0, half, rest), jnp.where(core == 0, rest, half)], axis=0
    )


def solution(mesh):
    in_specs = (P("dp", "row"), P("row"), P("row", None, "col"), P("col", "row"))
    out_specs = P("dp", "row")
    return jax.shard_map(shards, mesh=mesh, in_specs=in_specs, out_specs=out_specs, check_vma=False)
```

```python
import math

import jax
import jax.numpy as jnp
from jax import lax
from jax.experimental import pallas as pl
from jax.experimental.pallas import tpu as pltpu
from jax.sharding import PartitionSpec as P

K = 128
EPSILON = 1e-05
EXTRA = 128
HALF = 64
LIMIT = pltpu.CompilerParams(vmem_limit_bytes=20 * 2**20)

CLASSES = 4
NEAR = [[8 * y + 2 * i + b for y in range(2) for b in range(2)] for i in range(4)]
FAR = [[8 * y + 2 * i + b for i in range(4)] for y in range(2) for b in range(2)]
CORES = [(c, c ^ 1) for c in range(8)]
CHIPS = [[0, 2, 4, 6], [1, 3, 5, 7]]


def rounded(a):
    return a.astype(jnp.bfloat16).astype(jnp.float32)


def dot32(a, b):
    return jnp.dot(a, b, preferred_element_type=jnp.float32)


def with_statistics(base, columns):
    lane = lax.broadcasted_iota(jnp.int32, base.shape, 1)
    middle, total, square = columns
    for at, column in enumerate(
        (middle, rounded(total), total - rounded(total), rounded(square), square - rounded(square))
    ):
        base = jnp.where(lane == at, column, base)
    return base.astype(jnp.bfloat16)


def statistics(extra):
    return extra[:, 0:1], extra[:, 1:2] + extra[:, 2:3], extra[:, 3:4] + extra[:, 4:5]


def partial_kernel(per, x_ref, g_ref, w_ref, o_ref):
    tokens, width = x_ref.shape
    columns = w_ref.shape[2]
    values = x_ref[...].astype(jnp.float32)
    middle = rounded(jnp.sum(values, axis=1, keepdims=True) / width)
    centered = values - middle
    total = jnp.sum(centered, axis=1, keepdims=True)
    square = jnp.sum(centered * centered, axis=1, keepdims=True)
    gain = g_ref[...].reshape(1, width)
    scaled = (centered * gain).astype(jnp.bfloat16)
    high = rounded(gain)
    line = lax.broadcasted_iota(jnp.int32, (16, width), 0)
    gains = jnp.where(line == 0, high, jnp.where(line == 1, gain - high, 0.0)).astype(jnp.bfloat16)
    row = lax.broadcasted_iota(jnp.int32, (per, EXTRA), 0)
    sums = jnp.zeros((per, EXTRA), jnp.float32)
    chunk = 0
    chunks = 3 * columns // EXTRA
    for part in range(3):
        weight = w_ref[part]
        o_ref[:, part * columns : (part + 1) * columns] = dot32(scaled, weight).astype(jnp.bfloat16)
        c = jnp.sum(dot32(gains, weight), axis=0, keepdims=True)
        for at in range(0, columns, EXTRA):
            piece = c[:, at : at + EXTRA]
            sums = jnp.where(row == chunk, piece, sums)
            sums = jnp.where(row == chunks + chunk, pltpu.roll(piece, HALF, 1), sums)
            chunk += 1
    base = jnp.concatenate([sums] * (tokens // per), axis=0)
    o_ref[:, 3 * columns :] = with_statistics(base, (middle, total, square))


def vector_sums(extras, chunks):
    upper = lax.broadcasted_iota(jnp.int32, (1, EXTRA), 1) >= HALF
    turned = [pltpu.roll(e, HALF, 1) for e in extras]
    return [
        [
            jnp.where(upper, e[at : at + 1], t[chunks + at : chunks + at + 1])
            for e, t in zip(extras, turned)
        ]
        for at in range(chunks)
    ]


def merge_kernel(per, width, r_ref, o_ref):
    terms = [r_ref.at[d] for d in range(r_ref.shape[0])]
    size = o_ref.shape[0]
    columns = o_ref.shape[1] - EXTRA
    chunks = columns // EXTRA
    extras = [t[:, columns:].astype(jnp.float32) for t in terms]
    held = [statistics(e) for e in extras]
    middle = rounded(sum(m + t / width for m, t, _ in held) / len(terms))
    shifts = [m - middle for m, _, _ in held]
    total = sum(t + width * s for s, (_, t, _) in zip(shifts, held))
    square = sum(q + 2.0 * s * t + width * (s * s) for s, (_, t, q) in zip(shifts, held))
    pieces = vector_sums([e[:per] for e in extras], chunks)
    wide = [jnp.broadcast_to(s, (size, EXTRA)) for s in shifts]
    for at in range(chunks):
        running = jnp.zeros((size, EXTRA), jnp.float32)
        for t, w, c in zip(terms, wide, pieces[at]):
            running = running + t[:, at * EXTRA : (at + 1) * EXTRA].astype(jnp.float32) + w * c
        o_ref[:, at * EXTRA : (at + 1) * EXTRA] = running.astype(jnp.bfloat16)
    lines = sum(e[:per] for e in extras)
    base = jnp.concatenate([lines] * (size // per), axis=0)
    o_ref[:, columns:] = with_statistics(base, (middle, total, square))


def norm_kernel(width, r_ref, o_ref):
    blocks, per, _ = r_ref.shape
    columns = o_ref.shape[1]
    chunks = columns // EXTRA
    extras = [r_ref[d, :, columns:].astype(jnp.float32) for d in range(blocks)]
    held = [statistics(e) for e in extras]
    average = sum(m + t / width for m, t, _ in held) / blocks
    shifts = [m - average for m, _, _ in held]
    variance = sum(
        q + 2.0 * s * t + width * (s * s) for s, (_, t, q) in zip(shifts, held)
    ) / (width * blocks)
    scale = lax.rsqrt(variance + EPSILON)
    wide = [jnp.broadcast_to(s, (per, EXTRA)) for s in shifts]
    pieces = vector_sums(extras, chunks)
    for at in range(chunks):
        running = jnp.zeros((per, EXTRA), jnp.float32)
        for d in range(blocks):
            term = r_ref[d, :, at * EXTRA : (at + 1) * EXTRA].astype(jnp.float32)
            running = running + term + wide[d] * pieces[at][d]
        o_ref[:, at * EXTRA : (at + 1) * EXTRA] = (running * scale).astype(jnp.bfloat16)


def attend_kernel(x_ref, w_ref, keep_ref, send_ref, whole_ref):
    columns = w_ref.shape[0]
    scaling = 1.0 / math.sqrt(K)
    outs = []
    for at in range(0, columns, K):
        q = x_ref[:, at : at + K]
        k = x_ref[:, columns + at : columns + at + K]
        v = x_ref[:, 2 * columns + at : 2 * columns + at + K]
        scores = (
            lax.dot_general(q, k, (((1,), (1,)), ((), ())), preferred_element_type=jnp.float32)
            * scaling
        )
        largest = jnp.max(scores, axis=1, keepdims=True)
        exponent = jnp.exp(scores - largest)
        inverse = 1.0 / jnp.sum(exponent, axis=1, keepdims=True)
        outs.append(dot32((exponent * inverse).astype(jnp.bfloat16), v).astype(jnp.bfloat16))
    whole_ref[...] = dot32(jnp.concatenate(outs, axis=1), w_ref[...]).astype(jnp.bfloat16)
    half = keep_ref.shape[0]
    core = lax.rem(lax.axis_index("col"), 2)
    keep_ref[...] = whole_ref[pl.ds(pl.multiple_of(core * half, half), half), :]
    send_ref[...] = whole_ref[pl.ds(pl.multiple_of((1 - core) * half, half), half), :]


def exchange(a, axis, groups):
    return lax.all_to_all(a, axis, 0, 0, tiled=True, axis_index_groups=groups)


def spread(a, axis, groups):
    return exchange(jnp.broadcast_to(a[None], (len(groups[0]), *a.shape)), axis, groups)


def like(shape):
    return jax.ShapeDtypeStruct(shape, jnp.bfloat16)


def shards(tokens, norm_gain, qkv_weight, out_weight):
    count, width = tokens.shape
    columns = qkv_weight.shape[2]
    size = count // CLASSES
    per = size // len(FAR[0])
    wide = 3 * columns + EXTRA
    payload = pl.pallas_call(
        lambda *refs: partial_kernel(per, *refs),
        out_shape=like((count, wide)),
        name="partial",
        compiler_params=LIMIT,
    )(tokens, norm_gain, jnp.transpose(qkv_weight, (1, 0, 2)))
    near = exchange(payload.reshape(CLASSES, size, wide), "row", NEAR)
    merged = pl.pallas_call(
        lambda *refs: merge_kernel(per, width, *refs),
        out_shape=like((size, wide)),
        name="merge",
        compiler_params=LIMIT,
    )(near)
    far = exchange(merged.reshape(-1, per, wide), "row", FAR)
    mine = pl.pallas_call(
        lambda *refs: norm_kernel(width * CLASSES, *refs),
        out_shape=like((per, 3 * columns)),
        name="norm",
        compiler_params=LIMIT,
    )(far)
    block = spread(mine, "row", FAR).reshape(size, 3 * columns)
    qkv = spread(block, "row", NEAR).reshape(count, 3 * columns)
    keep, send = pl.pallas_call(
        attend_kernel,
        out_shape=[like((count // 2, width))] * 2,
        scratch_shapes=[pltpu.VMEM((count, width), jnp.bfloat16)],
        name="attend",
        compiler_params=LIMIT,
    )(qkv, out_weight)
    other = lax.ppermute(send, "col", CORES)
    pair = (keep.astype(jnp.float32) + other.astype(jnp.float32)).astype(jnp.bfloat16)
    terms = spread(pair, "col", CHIPS)
    half = jnp.sum(terms.astype(jnp.float32), axis=0).astype(jnp.bfloat16)
    rest = lax.ppermute(half, "col", CORES)
    core = lax.rem(lax.axis_index("col"), 2)
    return jnp.concatenate(
        [jnp.where(core == 0, half, rest), jnp.where(core == 0, rest, half)], axis=0
    )


def solution(mesh):
    in_specs = (P("dp", "row"), P("row"), P("row", None, "col"), P("col", "row"))
    out_specs = P("dp", "row")
    return jax.shard_map(shards, mesh=mesh, in_specs=in_specs, out_specs=out_specs, check_vma=False)
```

```python
import math

import jax
import jax.numpy as jnp
from jax import lax
from jax.experimental import pallas as pl
from jax.experimental.pallas import tpu as pltpu
from jax.sharding import PartitionSpec as P

K = 128
EPSILON = 1e-05
EXTRA = 128
HALF = 64
FIRST = pltpu.CompilerParams(vmem_limit_bytes=20 * 2**20)
LIMIT = pltpu.CompilerParams(vmem_limit_bytes=20 * 2**20)

CLASSES = 4
NEAR = [[8 * y + 2 * i + b for y in range(2) for b in range(2)] for i in range(4)]
FAR = [[8 * y + 2 * i + b for i in range(4)] for y in range(2) for b in range(2)]
CORES = [(c, c ^ 1) for c in range(8)]
RIGHT = [(c, c ^ 2) for c in range(8)]
LEFT = [(c, (c - 2 if c & 2 == 0 else c + 2) % 8) for c in range(8)]


def rounded(a):
    return a.astype(jnp.bfloat16).astype(jnp.float32)


def dot32(a, b):
    return jnp.dot(a, b, preferred_element_type=jnp.float32)


def with_statistics(base, columns):
    lane = lax.broadcasted_iota(jnp.int32, base.shape, 1)
    middle, total, square = columns
    for at, column in enumerate(
        (middle, rounded(total), total - rounded(total), rounded(square), square - rounded(square))
    ):
        base = jnp.where(lane == at, column, base)
    return base.astype(jnp.bfloat16)


def statistics(extra):
    return extra[:, 0:1], extra[:, 1:2] + extra[:, 2:3], extra[:, 3:4] + extra[:, 4:5]


def partial_kernel(per, x_ref, g_ref, w_ref, o_ref):
    tokens, width = x_ref.shape
    columns = w_ref.shape[2]
    values = x_ref[...].astype(jnp.float32)
    middle = rounded(jnp.sum(values, axis=1, keepdims=True) / width)
    centered = values - middle
    total = jnp.sum(centered, axis=1, keepdims=True)
    square = jnp.sum(centered * centered, axis=1, keepdims=True)
    gain = g_ref[...].reshape(1, width)
    scaled = (centered * gain).astype(jnp.bfloat16)
    high = rounded(gain)
    line = lax.broadcasted_iota(jnp.int32, (16, width), 0)
    gains = jnp.where(line == 0, high, jnp.where(line == 1, gain - high, 0.0)).astype(jnp.bfloat16)
    row = lax.broadcasted_iota(jnp.int32, (per, EXTRA), 0)
    sums = jnp.zeros((per, EXTRA), jnp.float32)
    chunk = 0
    chunks = 3 * columns // EXTRA
    for part in range(3):
        weight = w_ref[part]
        o_ref[:, part * columns : (part + 1) * columns] = dot32(scaled, weight).astype(jnp.bfloat16)
        c = jnp.sum(dot32(gains, weight), axis=0, keepdims=True)
        for at in range(0, columns, EXTRA):
            piece = c[:, at : at + EXTRA]
            sums = jnp.where(row == chunk, piece, sums)
            sums = jnp.where(row == chunks + chunk, pltpu.roll(piece, HALF, 1), sums)
            chunk += 1
    base = jnp.concatenate([sums] * (tokens // per), axis=0)
    o_ref[:, 3 * columns :] = with_statistics(base, (middle, total, square))


def vector_sums(extras, chunks):
    upper = lax.broadcasted_iota(jnp.int32, (1, EXTRA), 1) >= HALF
    turned = [pltpu.roll(e, HALF, 1) for e in extras]
    return [
        [
            jnp.where(upper, e[at : at + 1], t[chunks + at : chunks + at + 1])
            for e, t in zip(extras, turned)
        ]
        for at in range(chunks)
    ]


def merge_kernel(per, width, r_ref, o_ref):
    terms = [r_ref.at[d] for d in range(r_ref.shape[0])]
    size = o_ref.shape[0]
    columns = o_ref.shape[1] - EXTRA
    chunks = columns // EXTRA
    extras = [t[:, columns:].astype(jnp.float32) for t in terms]
    held = [statistics(e) for e in extras]
    middle = rounded(sum(m + t / width for m, t, _ in held) / len(terms))
    shifts = [m - middle for m, _, _ in held]
    total = sum(t + width * s for s, (_, t, _) in zip(shifts, held))
    square = sum(q + 2.0 * s * t + width * (s * s) for s, (_, t, q) in zip(shifts, held))
    pieces = vector_sums([e[:per] for e in extras], chunks)
    wide = [jnp.broadcast_to(s, (size, EXTRA)) for s in shifts]
    for at in range(chunks):
        running = jnp.zeros((size, EXTRA), jnp.float32)
        for t, w, c in zip(terms, wide, pieces[at]):
            running = running + t[:, at * EXTRA : (at + 1) * EXTRA].astype(jnp.float32) + w * c
        o_ref[:, at * EXTRA : (at + 1) * EXTRA] = running.astype(jnp.bfloat16)
    lines = sum(e[:per] for e in extras)
    base = jnp.concatenate([lines] * (size // per), axis=0)
    o_ref[:, columns:] = with_statistics(base, (middle, total, square))


def norm_kernel(width, r_ref, o_ref):
    blocks, per, _ = r_ref.shape
    columns = o_ref.shape[1]
    chunks = columns // EXTRA
    extras = [r_ref[d, :, columns:].astype(jnp.float32) for d in range(blocks)]
    held = [statistics(e) for e in extras]
    average = sum(m + t / width for m, t, _ in held) / blocks
    shifts = [m - average for m, _, _ in held]
    variance = sum(
        q + 2.0 * s * t + width * (s * s) for s, (_, t, q) in zip(shifts, held)
    ) / (width * blocks)
    scale = lax.rsqrt(variance + EPSILON)
    wide = [jnp.broadcast_to(s, (per, EXTRA)) for s in shifts]
    pieces = vector_sums(extras, chunks)
    for at in range(chunks):
        running = jnp.zeros((per, EXTRA), jnp.float32)
        for d in range(blocks):
            term = r_ref[d, :, at * EXTRA : (at + 1) * EXTRA].astype(jnp.float32)
            running = running + term + wide[d] * pieces[at][d]
        o_ref[:, at * EXTRA : (at + 1) * EXTRA] = (running * scale).astype(jnp.bfloat16)


def attend_kernel(other, x_ref, w_ref, o_ref):
    columns = w_ref.shape[0]
    half = o_ref.shape[0]
    core = lax.rem(lax.axis_index("col"), 2)
    which = 1 - core if other else core
    lines = pl.ds(pl.multiple_of(which * half, half), half)
    scaling = 1.0 / math.sqrt(K)
    outs = []
    for at in range(0, columns, K):
        q = x_ref[lines, at : at + K]
        k = x_ref[:, columns + at : columns + at + K]
        v = x_ref[:, 2 * columns + at : 2 * columns + at + K]
        scores = (
            lax.dot_general(q, k, (((1,), (1,)), ((), ())), preferred_element_type=jnp.float32)
            * scaling
        )
        largest = jnp.max(scores, axis=1, keepdims=True)
        exponent = jnp.exp(scores - largest)
        inverse = 1.0 / jnp.sum(exponent, axis=1, keepdims=True)
        outs.append(dot32((exponent * inverse).astype(jnp.bfloat16), v).astype(jnp.bfloat16))
    o_ref[...] = dot32(jnp.concatenate(outs, axis=1), w_ref[...]).astype(jnp.bfloat16)


def attend(other, qkv, weight):
    count, wide = qkv.shape
    width = weight.shape[1]
    flops = 2 * (count // 2) * (2 * count * weight.shape[0] + weight.shape[0] * width)
    return pl.pallas_call(
        lambda *refs: attend_kernel(other, *refs),
        out_shape=like((count // 2, width)),
        name="attend",
        compiler_params=LIMIT,
        cost_estimate=pl.CostEstimate(
            flops=4 * flops, bytes_accessed=2 * count * wide, transcendentals=0
        ),
    )(qkv, weight)


def added(a, b):
    return (a.astype(jnp.float32) + b.astype(jnp.float32)).astype(jnp.bfloat16)


def exchange(a, axis, groups):
    return lax.all_to_all(a, axis, 0, 0, tiled=True, axis_index_groups=groups)


def spread(a, axis, groups):
    return exchange(jnp.broadcast_to(a[None], (len(groups[0]), *a.shape)), axis, groups)


def like(shape):
    return jax.ShapeDtypeStruct(shape, jnp.bfloat16)


def shards(tokens, norm_gain, qkv_weight, out_weight):
    count, width = tokens.shape
    columns = qkv_weight.shape[2]
    size = count // CLASSES
    per = size // len(FAR[0])
    wide = 3 * columns + EXTRA
    payload = pl.pallas_call(
        lambda *refs: partial_kernel(per, *refs),
        out_shape=like((count, wide)),
        name="partial",
        compiler_params=FIRST,
    )(tokens, norm_gain, jnp.transpose(qkv_weight, (1, 0, 2)))
    near = exchange(payload.reshape(CLASSES, size, wide), "row", NEAR)
    merged = pl.pallas_call(
        lambda *refs: merge_kernel(per, width, *refs),
        out_shape=like((size, wide)),
        name="merge",
        compiler_params=LIMIT,
    )(near)
    far = exchange(merged.reshape(-1, per, wide), "row", FAR)
    mine = pl.pallas_call(
        lambda *refs: norm_kernel(width * CLASSES, *refs),
        out_shape=like((per, 3 * columns)),
        name="norm",
        compiler_params=LIMIT,
    )(far)
    block = spread(mine, "row", FAR).reshape(size, 3 * columns)
    qkv = spread(block, "row", NEAR).reshape(count, 3 * columns)
    send = lax.ppermute(attend(True, qkv, out_weight), "col", CORES)
    pair = added(attend(False, qkv, out_weight), send)
    four = added(pair, lax.ppermute(pair, "col", RIGHT))
    half = added(four, lax.ppermute(four, "col", LEFT))
    rest = lax.ppermute(half, "col", CORES)
    core = lax.rem(lax.axis_index("col"), 2)
    return jnp.concatenate(
        [jnp.where(core == 0, half, rest), jnp.where(core == 0, rest, half)], axis=0
    )


def solution(mesh):
    in_specs = (P("dp", "row"), P("row"), P("row", None, "col"), P("col", "row"))
    out_specs = P("dp", "row")
    return jax.shard_map(shards, mesh=mesh, in_specs=in_specs, out_specs=out_specs, check_vma=False)
```

```python
import math

import jax
import jax.numpy as jnp
from jax import lax
from jax.experimental import pallas as pl
from jax.experimental.pallas import tpu as pltpu
from jax.sharding import PartitionSpec as P

K = 128
EPSILON = 1e-05
EXTRA = 128
HALF = 64
LIMIT = pltpu.CompilerParams(vmem_limit_bytes=20 * 2**20)

CLASSES = 4
NEAR = [[8 * y + 2 * i + b for y in range(2) for b in range(2)] for i in range(4)]
FAR = [[8 * y + 2 * i + b for i in range(4)] for y in range(2) for b in range(2)]
CORES = [(c, c ^ 1) for c in range(8)]
CHIPS = [[0, 2, 4, 6], [1, 3, 5, 7]]


def rounded(a):
    return a.astype(jnp.bfloat16).astype(jnp.float32)


def dot32(a, b):
    return jnp.dot(a, b, preferred_element_type=jnp.float32)


def with_statistics(base, columns):
    lane = lax.broadcasted_iota(jnp.int32, base.shape, 1)
    middle, total, square = columns
    for at, column in enumerate(
        (middle, rounded(total), total - rounded(total), rounded(square), square - rounded(square))
    ):
        base = jnp.where(lane == at, column, base)
    return base.astype(jnp.bfloat16)


def statistics(extra):
    return extra[:, 0:1], extra[:, 1:2] + extra[:, 2:3], extra[:, 3:4] + extra[:, 4:5]


def center_kernel(x_ref, g_ref, o_ref, s_ref):
    width = x_ref.shape[1]
    values = x_ref[...].astype(jnp.float32)
    middle = rounded(jnp.sum(values, axis=1, keepdims=True) / width)
    centered = values - middle
    total = jnp.sum(centered, axis=1, keepdims=True)
    square = jnp.sum(centered * centered, axis=1, keepdims=True)
    o_ref[...] = (centered * g_ref[...].reshape(1, width)).astype(jnp.bfloat16)
    s_ref[...] = with_statistics(jnp.zeros(s_ref.shape, jnp.float32), (middle, total, square))


def partial_kernel(per, x_ref, s_ref, g_ref, w_ref, o_ref):
    tokens, width = x_ref.shape
    columns = w_ref.shape[2]
    gain = g_ref[...].reshape(1, width)
    scaled = x_ref[...]
    high = rounded(gain)
    line = lax.broadcasted_iota(jnp.int32, (16, width), 0)
    gains = jnp.where(line == 0, high, jnp.where(line == 1, gain - high, 0.0)).astype(jnp.bfloat16)
    row = lax.broadcasted_iota(jnp.int32, (per, EXTRA), 0)
    sums = jnp.zeros((per, EXTRA), jnp.float32)
    chunk = 0
    chunks = 3 * columns // EXTRA
    for part in range(3):
        weight = w_ref[part]
        o_ref[:, part * columns : (part + 1) * columns] = dot32(scaled, weight).astype(jnp.bfloat16)
        c = jnp.sum(dot32(gains, weight), axis=0, keepdims=True)
        for at in range(0, columns, EXTRA):
            piece = c[:, at : at + EXTRA]
            sums = jnp.where(row == chunk, piece, sums)
            sums = jnp.where(row == chunks + chunk, pltpu.roll(piece, HALF, 1), sums)
            chunk += 1
    base = jnp.concatenate([sums] * (tokens // per), axis=0)
    upper = lax.broadcasted_iota(jnp.int32, base.shape, 1) >= HALF
    o_ref[:, 3 * columns :] = jnp.where(upper, base, s_ref[...].astype(jnp.float32)).astype(
        jnp.bfloat16
    )


def vector_sums(extras, chunks):
    upper = lax.broadcasted_iota(jnp.int32, (1, EXTRA), 1) >= HALF
    turned = [pltpu.roll(e, HALF, 1) for e in extras]
    return [
        [
            jnp.where(upper, e[at : at + 1], t[chunks + at : chunks + at + 1])
            for e, t in zip(extras, turned)
        ]
        for at in range(chunks)
    ]


def merge_kernel(per, width, r_ref, o_ref):
    terms = [r_ref.at[d] for d in range(r_ref.shape[0])]
    size = o_ref.shape[0]
    columns = o_ref.shape[1] - EXTRA
    chunks = columns // EXTRA
    extras = [t[:, columns:].astype(jnp.float32) for t in terms]
    held = [statistics(e) for e in extras]
    middle = rounded(sum(m + t / width for m, t, _ in held) / len(terms))
    shifts = [m - middle for m, _, _ in held]
    total = sum(t + width * s for s, (_, t, _) in zip(shifts, held))
    square = sum(q + 2.0 * s * t + width * (s * s) for s, (_, t, q) in zip(shifts, held))
    pieces = vector_sums([e[:per] for e in extras], chunks)
    wide = [jnp.broadcast_to(s, (size, EXTRA)) for s in shifts]
    for at in range(chunks):
        running = jnp.zeros((size, EXTRA), jnp.float32)
        for t, w, c in zip(terms, wide, pieces[at]):
            running = running + t[:, at * EXTRA : (at + 1) * EXTRA].astype(jnp.float32) + w * c
        o_ref[:, at * EXTRA : (at + 1) * EXTRA] = running.astype(jnp.bfloat16)
    lines = sum(e[:per] for e in extras)
    base = jnp.concatenate([lines] * (size // per), axis=0)
    o_ref[:, columns:] = with_statistics(base, (middle, total, square))


def norm_kernel(width, r_ref, o_ref):
    blocks, per, _ = r_ref.shape
    columns = o_ref.shape[1]
    chunks = columns // EXTRA
    extras = [r_ref[d, :, columns:].astype(jnp.float32) for d in range(blocks)]
    held = [statistics(e) for e in extras]
    average = sum(m + t / width for m, t, _ in held) / blocks
    shifts = [m - average for m, _, _ in held]
    variance = sum(
        q + 2.0 * s * t + width * (s * s) for s, (_, t, q) in zip(shifts, held)
    ) / (width * blocks)
    scale = lax.rsqrt(variance + EPSILON)
    wide = [jnp.broadcast_to(s, (per, EXTRA)) for s in shifts]
    pieces = vector_sums(extras, chunks)
    for at in range(chunks):
        running = jnp.zeros((per, EXTRA), jnp.float32)
        for d in range(blocks):
            term = r_ref[d, :, at * EXTRA : (at + 1) * EXTRA].astype(jnp.float32)
            running = running + term + wide[d] * pieces[at][d]
        o_ref[:, at * EXTRA : (at + 1) * EXTRA] = (running * scale).astype(jnp.bfloat16)


def attend_kernel(other, x_ref, w_ref, o_ref):
    columns = w_ref.shape[0]
    half = o_ref.shape[0]
    core = lax.rem(lax.axis_index("col"), 2)
    which = 1 - core if other else core
    lines = pl.ds(pl.multiple_of(which * half, half), half)
    scaling = 1.0 / math.sqrt(K)
    outs = []
    for at in range(0, columns, K):
        q = x_ref[lines, at : at + K]
        k = x_ref[:, columns + at : columns + at + K]
        v = x_ref[:, 2 * columns + at : 2 * columns + at + K]
        scores = (
            lax.dot_general(q, k, (((1,), (1,)), ((), ())), preferred_element_type=jnp.float32)
            * scaling
        )
        largest = jnp.max(scores, axis=1, keepdims=True)
        exponent = jnp.exp(scores - largest)
        inverse = 1.0 / jnp.sum(exponent, axis=1, keepdims=True)
        outs.append(dot32((exponent * inverse).astype(jnp.bfloat16), v).astype(jnp.bfloat16))
    o_ref[...] = dot32(jnp.concatenate(outs, axis=1), w_ref[...]).astype(jnp.bfloat16)


def attend(other, qkv, weight):
    count, wide = qkv.shape
    width = weight.shape[1]
    flops = 2 * (count // 2) * (2 * count * weight.shape[0] + weight.shape[0] * width)
    return pl.pallas_call(
        lambda *refs: attend_kernel(other, *refs),
        out_shape=like((count // 2, width)),
        name="attend",
        compiler_params=LIMIT,
        cost_estimate=pl.CostEstimate(
            flops=4 * flops, bytes_accessed=2 * count * wide, transcendentals=0
        ),
    )(qkv, weight)


def added(a, b):
    return (a.astype(jnp.float32) + b.astype(jnp.float32)).astype(jnp.bfloat16)


def exchange(a, axis, groups):
    return lax.all_to_all(a, axis, 0, 0, tiled=True, axis_index_groups=groups)


def spread(a, axis, groups):
    return exchange(jnp.broadcast_to(a[None], (len(groups[0]), *a.shape)), axis, groups)


def like(shape):
    return jax.ShapeDtypeStruct(shape, jnp.bfloat16)


def shards(tokens, norm_gain, qkv_weight, out_weight):
    count, width = tokens.shape
    columns = qkv_weight.shape[2]
    size = count // CLASSES
    per = size // len(FAR[0])
    wide = 3 * columns + EXTRA
    scaled, kept = pl.pallas_call(
        center_kernel,
        out_shape=[like((count, width)), like((count, EXTRA))],
        name="center",
        compiler_params=LIMIT,
        cost_estimate=pl.CostEstimate(
            flops=2 * 10**9, bytes_accessed=4 * count * width, transcendentals=0
        ),
    )(tokens, norm_gain)
    payload = pl.pallas_call(
        lambda *refs: partial_kernel(per, *refs),
        out_shape=like((count, wide)),
        name="partial",
        compiler_params=LIMIT,
    )(scaled, kept, norm_gain, jnp.transpose(qkv_weight, (1, 0, 2)))
    near = exchange(payload.reshape(CLASSES, size, wide), "row", NEAR)
    merged = pl.pallas_call(
        lambda *refs: merge_kernel(per, width, *refs),
        out_shape=like((size, wide)),
        name="merge",
        compiler_params=LIMIT,
    )(near)
    far = exchange(merged.reshape(-1, per, wide), "row", FAR)
    mine = pl.pallas_call(
        lambda *refs: norm_kernel(width * CLASSES, *refs),
        out_shape=like((per, 3 * columns)),
        name="norm",
        compiler_params=LIMIT,
    )(far)
    block = spread(mine, "row", FAR).reshape(size, 3 * columns)
    qkv = spread(block, "row", NEAR).reshape(count, 3 * columns)
    send = lax.ppermute(attend(True, qkv, out_weight), "col", CORES)
    pair = added(attend(False, qkv, out_weight), send)
    terms = spread(pair, "col", CHIPS)
    half = jnp.sum(terms.astype(jnp.float32), axis=0).astype(jnp.bfloat16)
    rest = lax.ppermute(half, "col", CORES)
    core = lax.rem(lax.axis_index("col"), 2)
    return jnp.concatenate(
        [jnp.where(core == 0, half, rest), jnp.where(core == 0, rest, half)], axis=0
    )


def solution(mesh):
    in_specs = (P("dp", "row"), P("row"), P("row", None, "col"), P("col", "row"))
    out_specs = P("dp", "row")
    return jax.shard_map(shards, mesh=mesh, in_specs=in_specs, out_specs=out_specs, check_vma=False)
```

```python
import math

import jax
import jax.numpy as jnp
from jax import lax
from jax.experimental import pallas as pl
from jax.experimental.pallas import tpu as pltpu
from jax.sharding import PartitionSpec as P

K = 128
EPSILON = 1e-05
LANES = 128
HALF = 64
GROUP = 8
FIELDS = 5
TAIL = 16
LIMIT = pltpu.CompilerParams(vmem_limit_bytes=20 * 2**20)

CLASSES = 4
NEAR = [[8 * y + 2 * i + b for y in range(2) for b in range(2)] for i in range(4)]
FAR = [[8 * y + 2 * i + b for i in range(4)] for y in range(2) for b in range(2)]
CORES = [(c, c ^ 1) for c in range(8)]
CHIPS = [[0, 2, 4, 6], [1, 3, 5, 7]]


def rounded(a):
    return a.astype(jnp.bfloat16).astype(jnp.float32)


def dot32(a, b):
    return jnp.dot(a, b, preferred_element_type=jnp.float32)


def packed(columns):
    middle, total, square = columns
    tokens = middle.shape[0]
    fields = (
        middle, rounded(total), total - rounded(total), rounded(square), square - rounded(square)
    )
    lane = lax.broadcasted_iota(jnp.int32, (GROUP, LANES), 1)
    tile = jnp.zeros((GROUP, LANES), jnp.float32)
    for group in range(tokens // GROUP):
        for at, field in enumerate(fields):
            tile = jnp.where(
                lane == group * FIELDS + at, field[group * GROUP : (group + 1) * GROUP], tile
            )
    return tile


def unpacked(tile, tokens):
    groups = [
        tile if group == 0 else pltpu.roll(tile, LANES - group * FIELDS, 1)
        for group in range(tokens // GROUP)
    ]
    lines = jnp.concatenate(groups, axis=0)
    return lines[:, 0:1], lines[:, 1:2] + lines[:, 2:3], lines[:, 3:4] + lines[:, 4:5]


def tail_of(tile, sums):
    row = lax.broadcasted_iota(jnp.int32, (GROUP, LANES), 0)
    lane = lax.broadcasted_iota(jnp.int32, (GROUP, LANES), 1)
    first = jnp.zeros((GROUP, LANES), jnp.float32)
    for at in range(GROUP):
        first = jnp.where(row == at, sums[at], first)
    last = sums[GROUP]
    turned = pltpu.roll(last, HALF, 1)
    second = jnp.where(lane < HALF, tile, jnp.where(row == 0, last, turned))
    return jnp.concatenate([first, second], axis=0)


def sums_of(tail):
    upper = lax.broadcasted_iota(jnp.int32, (1, LANES), 1) >= HALF
    second = tail[GROUP:]
    turned = pltpu.roll(second, HALF, 1)
    return [tail[at : at + 1] for at in range(GROUP)] + [
        jnp.where(upper, second[0:1], turned[1:2])
    ]


def center_kernel(x_ref, o_ref, s_ref):
    count, width = x_ref.shape
    values = x_ref[...].astype(jnp.float32)
    middle = rounded(jnp.sum(values, axis=1, keepdims=True) / width)
    centered = values - middle
    total = jnp.sum(centered, axis=1, keepdims=True)
    square = jnp.sum(centered * centered, axis=1, keepdims=True)
    o_ref[...] = centered
    size = count // CLASSES
    for block in range(CLASSES):
        lines = slice(block * size, (block + 1) * size)
        s_ref[block] = packed((middle[lines], total[lines], square[lines]))


def partial_kernel(x_ref, s_ref, g_ref, w_ref, o_ref):
    tokens, width = x_ref.shape
    size = tokens // CLASSES
    columns = w_ref.shape[2]
    gain = g_ref[...].reshape(1, width)
    scaled = (x_ref[...] * gain).astype(jnp.bfloat16)
    high = rounded(gain)
    line = lax.broadcasted_iota(jnp.int32, (16, width), 0)
    gains = jnp.where(line == 0, high, jnp.where(line == 1, gain - high, 0.0)).astype(jnp.bfloat16)
    sums = []
    for part in range(3):
        weight = w_ref[part]
        product = dot32(scaled, weight).astype(jnp.bfloat16)
        c = jnp.sum(dot32(gains, weight), axis=0, keepdims=True)
        for at in range(0, columns, LANES):
            to = len(sums) * size
            for block in range(CLASSES):
                o_ref[block, to : to + size, :] = product[
                    block * size : (block + 1) * size, at : at + LANES
                ]
            sums.append(c[:, at : at + LANES])
    for block in range(CLASSES):
        o_ref[block, len(sums) * size :, :] = tail_of(s_ref[block], sums).astype(jnp.bfloat16)


def merge_kernel(width, r_ref, o_ref):
    blocks = r_ref.shape[0]
    members, rows, _ = o_ref.shape
    chunks = GROUP + 1
    per = (rows - TAIL) // chunks
    size = per * members
    tails = [r_ref[d, chunks * size :, :].astype(jnp.float32) for d in range(blocks)]
    held = [unpacked(t[GROUP:], size) for t in tails]
    middle = rounded(sum(m + t / width for m, t, _ in held) / blocks)
    shifts = [m - middle for m, _, _ in held]
    total = sum(t + width * s for s, (_, t, _) in zip(shifts, held))
    square = sum(q + 2.0 * s * t + width * (s * s) for s, (_, t, q) in zip(shifts, held))
    sums = [sums_of(t) for t in tails]
    wide = [jnp.broadcast_to(s, (size, LANES)) for s in shifts]
    for at in range(chunks):
        running = jnp.zeros((size, LANES), jnp.float32)
        for d in range(blocks):
            term = r_ref[d, at * size : (at + 1) * size, :].astype(jnp.float32)
            running = running + term + wide[d] * sums[d][at]
        result = running.astype(jnp.bfloat16)
        for member in range(members):
            o_ref[member, at * per : (at + 1) * per, :] = result[member * per : (member + 1) * per]
    merged = [sum(s[at] for s in sums) for at in range(chunks)]
    for member in range(members):
        lines = slice(member * per, (member + 1) * per)
        tile = packed((middle[lines], total[lines], square[lines]))
        o_ref[member, chunks * per :, :] = tail_of(tile, merged).astype(jnp.bfloat16)


def norm_kernel(width, r_ref, o_ref):
    blocks = r_ref.shape[0]
    per, columns = o_ref.shape
    chunks = columns // LANES
    tails = [r_ref[d, chunks * per :, :].astype(jnp.float32) for d in range(blocks)]
    held = [unpacked(t[GROUP:], per) for t in tails]
    average = sum(m + t / width for m, t, _ in held) / blocks
    shifts = [m - average for m, _, _ in held]
    variance = sum(
        q + 2.0 * s * t + width * (s * s) for s, (_, t, q) in zip(shifts, held)
    ) / (width * blocks)
    scale = lax.rsqrt(variance + EPSILON)
    wide = [jnp.broadcast_to(s, (per, LANES)) for s in shifts]
    sums = [sums_of(t) for t in tails]
    for at in range(chunks):
        running = jnp.zeros((per, LANES), jnp.float32)
        for d in range(blocks):
            term = r_ref[d, at * per : (at + 1) * per, :].astype(jnp.float32)
            running = running + term + wide[d] * sums[d][at]
        o_ref[:, at * LANES : (at + 1) * LANES] = (running * scale).astype(jnp.bfloat16)


def attend_kernel(other, x_ref, w_ref, o_ref):
    columns = w_ref.shape[0]
    half = o_ref.shape[0]
    core = lax.rem(lax.axis_index("col"), 2)
    which = 1 - core if other else core
    lines = pl.ds(pl.multiple_of(which * half, half), half)
    scaling = 1.0 / math.sqrt(K)
    outs = []
    for at in range(0, columns, K):
        q = x_ref[lines, at : at + K]
        k = x_ref[:, columns + at : columns + at + K]
        v = x_ref[:, 2 * columns + at : 2 * columns + at + K]
        scores = (
            lax.dot_general(q, k, (((1,), (1,)), ((), ())), preferred_element_type=jnp.float32)
            * scaling
        )
        largest = jnp.max(scores, axis=1, keepdims=True)
        exponent = jnp.exp(scores - largest)
        inverse = 1.0 / jnp.sum(exponent, axis=1, keepdims=True)
        outs.append(dot32((exponent * inverse).astype(jnp.bfloat16), v).astype(jnp.bfloat16))
    o_ref[...] = dot32(jnp.concatenate(outs, axis=1), w_ref[...]).astype(jnp.bfloat16)


def attend(other, qkv, weight):
    count, wide = qkv.shape
    width = weight.shape[1]
    flops = 2 * (count // 2) * (2 * count * weight.shape[0] + weight.shape[0] * width)
    return pl.pallas_call(
        lambda *refs: attend_kernel(other, *refs),
        out_shape=like((count // 2, width)),
        name="attend",
        compiler_params=LIMIT,
        cost_estimate=pl.CostEstimate(
            flops=4 * flops, bytes_accessed=2 * count * wide, transcendentals=0
        ),
    )(qkv, weight)


def added(a, b):
    return (a.astype(jnp.float32) + b.astype(jnp.float32)).astype(jnp.bfloat16)


def exchange(a, axis, groups):
    return lax.all_to_all(a, axis, 0, 0, tiled=True, axis_index_groups=groups)


def spread(a, axis, groups):
    return exchange(jnp.broadcast_to(a[None], (len(groups[0]), *a.shape)), axis, groups)


def like(shape):
    return jax.ShapeDtypeStruct(shape, jnp.bfloat16)


def shards(tokens, norm_gain, qkv_weight, out_weight):
    count, width = tokens.shape
    columns = qkv_weight.shape[2]
    size = count // CLASSES
    per = size // len(FAR[0])
    chunks = GROUP + 1
    centered, kept = pl.pallas_call(
        center_kernel,
        out_shape=[
            jax.ShapeDtypeStruct((count, width), jnp.float32),
            jax.ShapeDtypeStruct((CLASSES, GROUP, LANES), jnp.float32),
        ],
        name="center",
        compiler_params=LIMIT,
        cost_estimate=pl.CostEstimate(
            flops=2 * 10**9, bytes_accessed=4 * count * width, transcendentals=0
        ),
    )(tokens)
    payload = pl.pallas_call(
        partial_kernel,
        out_shape=like((CLASSES, chunks * size + TAIL, LANES)),
        name="partial",
        compiler_params=LIMIT,
    )(centered, kept, norm_gain, jnp.transpose(qkv_weight, (1, 0, 2)))
    near = exchange(payload, "row", NEAR)
    merged = pl.pallas_call(
        lambda *refs: merge_kernel(width, *refs),
        out_shape=like((len(FAR[0]), chunks * per + TAIL, LANES)),
        name="merge",
        compiler_params=LIMIT,
    )(near)
    far = exchange(merged, "row", FAR)
    mine = pl.pallas_call(
        lambda *refs: norm_kernel(width * CLASSES, *refs),
        out_shape=like((per, 3 * columns)),
        name="norm",
        compiler_params=LIMIT,
    )(far)
    block = spread(mine, "row", FAR).reshape(size, 3 * columns)
    qkv = spread(block, "row", NEAR).reshape(count, 3 * columns)
    send = lax.ppermute(attend(True, qkv, out_weight), "col", CORES)
    pair = added(attend(False, qkv, out_weight), send)
    terms = spread(pair, "col", CHIPS)
    half = jnp.sum(terms.astype(jnp.float32), axis=0).astype(jnp.bfloat16)
    rest = lax.ppermute(half, "col", CORES)
    core = lax.rem(lax.axis_index("col"), 2)
    return jnp.concatenate(
        [jnp.where(core == 0, half, rest), jnp.where(core == 0, rest, half)], axis=0
    )


def solution(mesh):
    in_specs = (P("dp", "row"), P("row"), P("row", None, "col"), P("col", "row"))
    out_specs = P("dp", "row")
    return jax.shard_map(shards, mesh=mesh, in_specs=in_specs, out_specs=out_specs, check_vma=False)
```

```python
import math

import jax
import jax.numpy as jnp
from jax import lax
from jax.experimental import pallas as pl
from jax.experimental.pallas import tpu as pltpu
from jax.sharding import PartitionSpec as P

K = 128
EPSILON = 1e-05
LANES = 128
HALF = 64
GROUP = 8
FIELDS = 5
TAIL = 16
LIMIT = pltpu.CompilerParams(vmem_limit_bytes=20 * 2**20)

CLASSES = 4
NEAR = [[8 * y + 2 * i + b for y in range(2) for b in range(2)] for i in range(4)]
FAR = [[8 * y + 2 * i + b for i in range(4)] for y in range(2) for b in range(2)]
CORES = [(c, c ^ 1) for c in range(8)]
CHIPS = [[0, 2, 4, 6], [1, 3, 5, 7]]


def rounded(a):
    return a.astype(jnp.bfloat16).astype(jnp.float32)


def dot32(a, b):
    return jnp.dot(a, b, preferred_element_type=jnp.float32)


def packed(columns):
    middle, total, square = columns
    tokens = middle.shape[0]
    fields = (
        middle, rounded(total), total - rounded(total), rounded(square), square - rounded(square)
    )
    lane = lax.broadcasted_iota(jnp.int32, (GROUP, LANES), 1)
    tile = jnp.zeros((GROUP, LANES), jnp.float32)
    for group in range(tokens // GROUP):
        for at, field in enumerate(fields):
            tile = jnp.where(
                lane == group * FIELDS + at, field[group * GROUP : (group + 1) * GROUP], tile
            )
    return tile


def moved(tile, lanes):
    return tile if lanes % LANES == 0 else pltpu.roll(tile, -lanes % LANES, 1)


def held_in(tile):
    return tile, moved(tile, 1) + moved(tile, 2), moved(tile, 3) + moved(tile, 4)


def fields_of(middle, total, square):
    lane = lax.broadcasted_iota(jnp.int32, (GROUP, LANES), 1)
    field = lax.rem(lane, FIELDS)
    tile = middle
    for at, number in enumerate(
        (rounded(total), total - rounded(total), rounded(square), square - rounded(square))
    ):
        tile = jnp.where(field == at + 1, moved(number, -1 - at), tile)
    return jnp.where(lane < HALF, tile, 0.0)


def lines_of(tile, tokens):
    return jnp.concatenate(
        [
            jnp.broadcast_to(tile[:, group * FIELDS : group * FIELDS + 1], (GROUP, LANES))
            for group in range(tokens // GROUP)
        ],
        axis=0,
    )


def tail_of(tile, sums):
    row = lax.broadcasted_iota(jnp.int32, (GROUP, LANES), 0)
    lane = lax.broadcasted_iota(jnp.int32, (GROUP, LANES), 1)
    first = jnp.zeros((GROUP, LANES), jnp.float32)
    for at in range(GROUP):
        first = jnp.where(row == at, sums[at], first)
    last = sums[GROUP]
    turned = pltpu.roll(last, HALF, 1)
    second = jnp.where(lane < HALF, tile, jnp.where(row == 0, last, turned))
    return jnp.concatenate([first, second], axis=0)


def sums_of(tail):
    upper = lax.broadcasted_iota(jnp.int32, (1, LANES), 1) >= HALF
    second = tail[GROUP:]
    turned = pltpu.roll(second, HALF, 1)
    return [tail[at : at + 1] for at in range(GROUP)] + [
        jnp.where(upper, second[0:1], turned[1:2])
    ]


def center_kernel(x_ref, o_ref, s_ref):
    count, width = x_ref.shape
    values = x_ref[...].astype(jnp.float32)
    middle = rounded(jnp.sum(values, axis=1, keepdims=True) / width)
    centered = values - middle
    total = jnp.sum(centered, axis=1, keepdims=True)
    square = jnp.sum(centered * centered, axis=1, keepdims=True)
    o_ref[...] = centered
    size = count // CLASSES
    for block in range(CLASSES):
        lines = slice(block * size, (block + 1) * size)
        s_ref[block] = packed((middle[lines], total[lines], square[lines]))


def partial_kernel(x_ref, s_ref, g_ref, w_ref, o_ref):
    tokens, width = x_ref.shape
    size = tokens // CLASSES
    columns = w_ref.shape[2]
    gain = g_ref[...].reshape(1, width)
    scaled = (x_ref[...] * gain).astype(jnp.bfloat16)
    high = rounded(gain)
    line = lax.broadcasted_iota(jnp.int32, (16, width), 0)
    gains = jnp.where(line == 0, high, jnp.where(line == 1, gain - high, 0.0)).astype(jnp.bfloat16)
    sums = []
    for part in range(3):
        weight = w_ref[part]
        product = dot32(scaled, weight).astype(jnp.bfloat16)
        c = jnp.sum(dot32(gains, weight), axis=0, keepdims=True)
        for at in range(0, columns, LANES):
            to = len(sums) * size
            for block in range(CLASSES):
                o_ref[block, to : to + size, :] = product[
                    block * size : (block + 1) * size, at : at + LANES
                ]
            sums.append(c[:, at : at + LANES])
    for block in range(CLASSES):
        o_ref[block, len(sums) * size :, :] = tail_of(s_ref[block], sums).astype(jnp.bfloat16)


def merge_kernel(width, r_ref, o_ref):
    blocks = r_ref.shape[0]
    members, rows, _ = o_ref.shape
    chunks = GROUP + 1
    per = (rows - TAIL) // chunks
    size = per * members
    tails = [r_ref[d, chunks * size :, :].astype(jnp.float32) for d in range(blocks)]
    held = [held_in(t[GROUP:]) for t in tails]
    middle = rounded(sum(m + t / width for m, t, _ in held) / blocks)
    shifts = [m - middle for m, _, _ in held]
    total = sum(t + width * s for s, (_, t, _) in zip(shifts, held))
    square = sum(q + 2.0 * s * t + width * (s * s) for s, (_, t, q) in zip(shifts, held))
    sums = [sums_of(t) for t in tails]
    wide = [lines_of(s, size) for s in shifts]
    for at in range(chunks):
        running = jnp.zeros((size, LANES), jnp.float32)
        for d in range(blocks):
            term = r_ref[d, at * size : (at + 1) * size, :].astype(jnp.float32)
            running = running + term + wide[d] * sums[d][at]
        result = running.astype(jnp.bfloat16)
        for member in range(members):
            o_ref[member, at * per : (at + 1) * per, :] = result[member * per : (member + 1) * per]
    merged = [sum(s[at] for s in sums) for at in range(chunks)]
    tile = fields_of(middle, total, square)
    for member in range(members):
        part = moved(tile, member * (per // GROUP) * FIELDS)
        o_ref[member, chunks * per :, :] = tail_of(part, merged).astype(jnp.bfloat16)


def norm_kernel(width, r_ref, o_ref):
    blocks = r_ref.shape[0]
    per, columns = o_ref.shape
    chunks = columns // LANES
    tails = [r_ref[d, chunks * per :, :].astype(jnp.float32) for d in range(blocks)]
    held = [held_in(t[GROUP:]) for t in tails]
    average = sum(m + t / width for m, t, _ in held) / blocks
    shifts = [m - average for m, _, _ in held]
    variance = sum(
        q + 2.0 * s * t + width * (s * s) for s, (_, t, q) in zip(shifts, held)
    ) / (width * blocks)
    scale = lines_of(lax.rsqrt(variance + EPSILON), per)
    wide = [lines_of(s, per) for s in shifts]
    sums = [sums_of(t) for t in tails]
    for at in range(chunks):
        running = jnp.zeros((per, LANES), jnp.float32)
        for d in range(blocks):
            term = r_ref[d, at * per : (at + 1) * per, :].astype(jnp.float32)
            running = running + term + wide[d] * sums[d][at]
        o_ref[:, at * LANES : (at + 1) * LANES] = (running * scale).astype(jnp.bfloat16)


def attend_kernel(other, x_ref, w_ref, o_ref):
    columns = w_ref.shape[0]
    half = o_ref.shape[0]
    core = lax.rem(lax.axis_index("col"), 2)
    which = 1 - core if other else core
    lines = pl.ds(pl.multiple_of(which * half, half), half)
    scaling = 1.0 / math.sqrt(K)
    starts = range(0, columns, K)
    scores = jnp.concatenate(
        [
            lax.dot_general(
                x_ref[lines, at : at + K],
                x_ref[:, columns + at : columns + at + K],
                (((1,), (1,)), ((), ())),
                preferred_element_type=jnp.float32,
            )
            for at in starts
        ],
        axis=0,
    )
    largest = jnp.max(scores, axis=1, keepdims=True)
    exponent = jnp.exp((scores - largest) * scaling)
    inverse = 1.0 / jnp.sum(exponent, axis=1, keepdims=True)
    shares = (exponent * inverse).astype(jnp.bfloat16)
    outs = [
        dot32(
            shares[head * half : (head + 1) * half],
            x_ref[:, 2 * columns + at : 2 * columns + at + K],
        ).astype(jnp.bfloat16)
        for head, at in enumerate(starts)
    ]
    o_ref[...] = dot32(jnp.concatenate(outs, axis=1), w_ref[...]).astype(jnp.bfloat16)


def attend(other, qkv, weight):
    count, wide = qkv.shape
    width = weight.shape[1]
    flops = 2 * (count // 2) * (2 * count * weight.shape[0] + weight.shape[0] * width)
    return pl.pallas_call(
        lambda *refs: attend_kernel(other, *refs),
        out_shape=like((count // 2, width)),
        name="attend",
        compiler_params=LIMIT,
        cost_estimate=pl.CostEstimate(
            flops=4 * flops, bytes_accessed=2 * count * wide, transcendentals=0
        ),
    )(qkv, weight)


def added(a, b):
    return (a.astype(jnp.float32) + b.astype(jnp.float32)).astype(jnp.bfloat16)


def exchange(a, axis, groups):
    return lax.all_to_all(a, axis, 0, 0, tiled=True, axis_index_groups=groups)


def spread(a, axis, groups):
    return exchange(jnp.broadcast_to(a[None], (len(groups[0]), *a.shape)), axis, groups)


def like(shape):
    return jax.ShapeDtypeStruct(shape, jnp.bfloat16)


def shards(tokens, norm_gain, qkv_weight, out_weight):
    count, width = tokens.shape
    columns = qkv_weight.shape[2]
    size = count // CLASSES
    per = size // len(FAR[0])
    chunks = GROUP + 1
    centered, kept = pl.pallas_call(
        center_kernel,
        out_shape=[
            jax.ShapeDtypeStruct((count, width), jnp.float32),
            jax.ShapeDtypeStruct((CLASSES, GROUP, LANES), jnp.float32),
        ],
        name="center",
        compiler_params=LIMIT,
        cost_estimate=pl.CostEstimate(
            flops=2 * 10**9, bytes_accessed=4 * count * width, transcendentals=0
        ),
    )(tokens)
    payload = pl.pallas_call(
        partial_kernel,
        out_shape=like((CLASSES, chunks * size + TAIL, LANES)),
        name="partial",
        compiler_params=LIMIT,
    )(centered, kept, norm_gain, jnp.transpose(qkv_weight, (1, 0, 2)))
    near = exchange(payload, "row", NEAR)
    merged = pl.pallas_call(
        lambda *refs: merge_kernel(width, *refs),
        out_shape=like((len(FAR[0]), chunks * per + TAIL, LANES)),
        name="merge",
        compiler_params=LIMIT,
    )(near)
    far = exchange(merged, "row", FAR)
    mine = pl.pallas_call(
        lambda *refs: norm_kernel(width * CLASSES, *refs),
        out_shape=like((per, 3 * columns)),
        name="norm",
        compiler_params=LIMIT,
    )(far)
    block = spread(mine, "row", FAR).reshape(size, 3 * columns)
    qkv = spread(block, "row", NEAR).reshape(count, 3 * columns)
    send = lax.ppermute(attend(True, qkv, out_weight), "col", CORES)
    pair = added(attend(False, qkv, out_weight), send)
    terms = spread(pair, "col", CHIPS)
    half = jnp.sum(terms.astype(jnp.float32), axis=0).astype(jnp.bfloat16)
    rest = lax.ppermute(half, "col", CORES)
    core = lax.rem(lax.axis_index("col"), 2)
    return jnp.concatenate(
        [jnp.where(core == 0, half, rest), jnp.where(core == 0, rest, half)], axis=0
    )


def solution(mesh):
    in_specs = (P("dp", "row"), P("row"), P("row", None, "col"), P("col", "row"))
    out_specs = P("dp", "row")
    return jax.shard_map(shards, mesh=mesh, in_specs=in_specs, out_specs=out_specs, check_vma=False)
```

```python
import math

import jax
import jax.numpy as jnp
from jax import lax
from jax.experimental import pallas as pl
from jax.experimental.pallas import tpu as pltpu
from jax.sharding import PartitionSpec as P

K = 128
EPSILON = 1e-05
LANES = 128
HALF = 64
GROUP = 8
FIELDS = 5
TAIL = 16
LIMIT = pltpu.CompilerParams(vmem_limit_bytes=20 * 2**20)

CLASSES = 4
PLACES = ((1, 2, 4, 7), (0, 3, 5, 6))
NEAR = [[8 * y + place[i] for y in range(2) for place in PLACES] for i in range(4)]
FAR = [[8 * y + z for z in place] for y in range(2) for place in PLACES]
CORES = [(c, c ^ 1) for c in range(8)]
CHIPS = [[0, 2, 4, 6], [1, 3, 5, 7]]


def rounded(a):
    return a.astype(jnp.bfloat16).astype(jnp.float32)


def dot32(a, b):
    return jnp.dot(a, b, preferred_element_type=jnp.float32)


def packed(columns):
    middle, total, square = columns
    tokens = middle.shape[0]
    fields = (
        middle, rounded(total), total - rounded(total), rounded(square), square - rounded(square)
    )
    lane = lax.broadcasted_iota(jnp.int32, (GROUP, LANES), 1)
    tile = jnp.zeros((GROUP, LANES), jnp.float32)
    for group in range(tokens // GROUP):
        for at, field in enumerate(fields):
            tile = jnp.where(
                lane == group * FIELDS + at, field[group * GROUP : (group + 1) * GROUP], tile
            )
    return tile


def moved(tile, lanes):
    return tile if lanes % LANES == 0 else pltpu.roll(tile, -lanes % LANES, 1)


def held_in(tile):
    return tile, moved(tile, 1) + moved(tile, 2), moved(tile, 3) + moved(tile, 4)


def fields_of(middle, total, square):
    lane = lax.broadcasted_iota(jnp.int32, (GROUP, LANES), 1)
    field = lax.rem(lane, FIELDS)
    tile = middle
    for at, number in enumerate(
        (rounded(total), total - rounded(total), rounded(square), square - rounded(square))
    ):
        tile = jnp.where(field == at + 1, moved(number, -1 - at), tile)
    return jnp.where(lane < HALF, tile, 0.0)


def lines_of(tile, tokens):
    return jnp.concatenate(
        [
            jnp.broadcast_to(tile[:, group * FIELDS : group * FIELDS + 1], (GROUP, LANES))
            for group in range(tokens // GROUP)
        ],
        axis=0,
    )


def tail_of(tile, sums):
    row = lax.broadcasted_iota(jnp.int32, (GROUP, LANES), 0)
    lane = lax.broadcasted_iota(jnp.int32, (GROUP, LANES), 1)
    first = jnp.zeros((GROUP, LANES), jnp.float32)
    for at in range(GROUP):
        first = jnp.where(row == at, sums[at], first)
    last = sums[GROUP]
    turned = pltpu.roll(last, HALF, 1)
    second = jnp.where(lane < HALF, tile, jnp.where(row == 0, last, turned))
    return jnp.concatenate([first, second], axis=0)


def sums_of(tail):
    upper = lax.broadcasted_iota(jnp.int32, (1, LANES), 1) >= HALF
    second = tail[GROUP:]
    turned = pltpu.roll(second, HALF, 1)
    return [tail[at : at + 1] for at in range(GROUP)] + [
        jnp.where(upper, second[0:1], turned[1:2])
    ]


def center_kernel(x_ref, o_ref, s_ref):
    count, width = x_ref.shape
    values = x_ref[...].astype(jnp.float32)
    middle = rounded(jnp.sum(values, axis=1, keepdims=True) / width)
    centered = values - middle
    total = jnp.sum(centered, axis=1, keepdims=True)
    square = jnp.sum(centered * centered, axis=1, keepdims=True)
    o_ref[...] = centered
    size = count // CLASSES
    for block in range(CLASSES):
        lines = slice(block * size, (block + 1) * size)
        s_ref[block] = packed((middle[lines], total[lines], square[lines]))


def partial_kernel(x_ref, s_ref, g_ref, w_ref, o_ref):
    tokens, width = x_ref.shape
    size = tokens // CLASSES
    columns = w_ref.shape[2]
    gain = g_ref[...].reshape(1, width)
    scaled = (x_ref[...] * gain).astype(jnp.bfloat16)
    high = rounded(gain)
    line = lax.broadcasted_iota(jnp.int32, (16, width), 0)
    gains = jnp.where(line == 0, high, jnp.where(line == 1, gain - high, 0.0)).astype(jnp.bfloat16)
    sums = []
    for part in range(3):
        weight = w_ref[part]
        product = dot32(scaled, weight).astype(jnp.bfloat16)
        c = jnp.sum(dot32(gains, weight), axis=0, keepdims=True)
        for at in range(0, columns, LANES):
            to = len(sums) * size
            for block in range(CLASSES):
                o_ref[block, to : to + size, :] = product[
                    block * size : (block + 1) * size, at : at + LANES
                ]
            sums.append(c[:, at : at + LANES])
    for block in range(CLASSES):
        o_ref[block, len(sums) * size :, :] = tail_of(s_ref[block], sums).astype(jnp.bfloat16)


def merge_kernel(width, r_ref, o_ref):
    blocks = r_ref.shape[0]
    members, rows, _ = o_ref.shape
    chunks = GROUP + 1
    per = (rows - TAIL) // chunks
    size = per * members
    tails = [r_ref[d, chunks * size :, :].astype(jnp.float32) for d in range(blocks)]
    held = [held_in(t[GROUP:]) for t in tails]
    middle = rounded(sum(m + t / width for m, t, _ in held) / blocks)
    shifts = [m - middle for m, _, _ in held]
    total = sum(t + width * s for s, (_, t, _) in zip(shifts, held))
    square = sum(q + 2.0 * s * t + width * (s * s) for s, (_, t, q) in zip(shifts, held))
    sums = [sums_of(t) for t in tails]
    wide = [lines_of(s, size) for s in shifts]
    for at in range(chunks):
        running = jnp.zeros((size, LANES), jnp.float32)
        for d in range(blocks):
            term = r_ref[d, at * size : (at + 1) * size, :].astype(jnp.float32)
            running = running + term + wide[d] * sums[d][at]
        result = running.astype(jnp.bfloat16)
        for member in range(members):
            o_ref[member, at * per : (at + 1) * per, :] = result[member * per : (member + 1) * per]
    merged = [sum(s[at] for s in sums) for at in range(chunks)]
    tile = fields_of(middle, total, square)
    for member in range(members):
        part = moved(tile, member * (per // GROUP) * FIELDS)
        o_ref[member, chunks * per :, :] = tail_of(part, merged).astype(jnp.bfloat16)


def norm_kernel(width, r_ref, o_ref):
    blocks = r_ref.shape[0]
    per, columns = o_ref.shape
    chunks = columns // LANES
    tails = [r_ref[d, chunks * per :, :].astype(jnp.float32) for d in range(blocks)]
    held = [held_in(t[GROUP:]) for t in tails]
    average = sum(m + t / width for m, t, _ in held) / blocks
    shifts = [m - average for m, _, _ in held]
    variance = sum(
        q + 2.0 * s * t + width * (s * s) for s, (_, t, q) in zip(shifts, held)
    ) / (width * blocks)
    scale = lines_of(lax.rsqrt(variance + EPSILON), per)
    wide = [lines_of(s, per) for s in shifts]
    sums = [sums_of(t) for t in tails]
    for at in range(chunks):
        running = jnp.zeros((per, LANES), jnp.float32)
        for d in range(blocks):
            term = r_ref[d, at * per : (at + 1) * per, :].astype(jnp.float32)
            running = running + term + wide[d] * sums[d][at]
        o_ref[:, at * LANES : (at + 1) * LANES] = (running * scale).astype(jnp.bfloat16)


def attend_kernel(other, x_ref, w_ref, o_ref):
    columns = w_ref.shape[0]
    half = o_ref.shape[0]
    core = lax.rem(lax.axis_index("col"), 2)
    which = 1 - core if other else core
    lines = pl.ds(pl.multiple_of(which * half, half), half)
    scaling = 1.0 / math.sqrt(K)
    starts = range(0, columns, K)
    scores = jnp.concatenate(
        [
            lax.dot_general(
                x_ref[lines, at : at + K],
                x_ref[:, columns + at : columns + at + K],
                (((1,), (1,)), ((), ())),
                preferred_element_type=jnp.float32,
            )
            for at in starts
        ],
        axis=0,
    )
    largest = jnp.max(scores, axis=1, keepdims=True)
    exponent = jnp.exp((scores - largest) * scaling)
    inverse = 1.0 / jnp.sum(exponent, axis=1, keepdims=True)
    shares = (exponent * inverse).astype(jnp.bfloat16)
    outs = [
        dot32(
            shares[head * half : (head + 1) * half],
            x_ref[:, 2 * columns + at : 2 * columns + at + K],
        ).astype(jnp.bfloat16)
        for head, at in enumerate(starts)
    ]
    o_ref[...] = dot32(jnp.concatenate(outs, axis=1), w_ref[...]).astype(jnp.bfloat16)


def attend(other, qkv, weight):
    count, wide = qkv.shape
    width = weight.shape[1]
    flops = 2 * (count // 2) * (2 * count * weight.shape[0] + weight.shape[0] * width)
    return pl.pallas_call(
        lambda *refs: attend_kernel(other, *refs),
        out_shape=like((count // 2, width)),
        name="attend",
        compiler_params=LIMIT,
        cost_estimate=pl.CostEstimate(
            flops=4 * flops, bytes_accessed=2 * count * wide, transcendentals=0
        ),
    )(qkv, weight)


def added(a, b):
    return (a.astype(jnp.float32) + b.astype(jnp.float32)).astype(jnp.bfloat16)


def exchange(a, axis, groups):
    return lax.all_to_all(a, axis, 0, 0, tiled=True, axis_index_groups=groups)


def spread(a, axis, groups):
    return exchange(jnp.broadcast_to(a[None], (len(groups[0]), *a.shape)), axis, groups)


def like(shape):
    return jax.ShapeDtypeStruct(shape, jnp.bfloat16)


def shards(tokens, norm_gain, qkv_weight, out_weight):
    count, width = tokens.shape
    columns = qkv_weight.shape[2]
    size = count // CLASSES
    per = size // len(FAR[0])
    chunks = GROUP + 1
    centered, kept = pl.pallas_call(
        center_kernel,
        out_shape=[
            jax.ShapeDtypeStruct((count, width), jnp.float32),
            jax.ShapeDtypeStruct((CLASSES, GROUP, LANES), jnp.float32),
        ],
        name="center",
        compiler_params=LIMIT,
        cost_estimate=pl.CostEstimate(
            flops=2 * 10**9, bytes_accessed=4 * count * width, transcendentals=0
        ),
    )(tokens)
    payload = pl.pallas_call(
        partial_kernel,
        out_shape=like((CLASSES, chunks * size + TAIL, LANES)),
        name="partial",
        compiler_params=LIMIT,
    )(centered, kept, norm_gain, jnp.transpose(qkv_weight, (1, 0, 2)))
    near = exchange(payload, "row", NEAR)
    merged = pl.pallas_call(
        lambda *refs: merge_kernel(width, *refs),
        out_shape=like((len(FAR[0]), chunks * per + TAIL, LANES)),
        name="merge",
        compiler_params=LIMIT,
    )(near)
    far = exchange(merged, "row", FAR)
    mine = pl.pallas_call(
        lambda *refs: norm_kernel(width * CLASSES, *refs),
        out_shape=like((per, 3 * columns)),
        name="norm",
        compiler_params=LIMIT,
    )(far)
    block = spread(mine, "row", FAR).reshape(size, 3 * columns)
    qkv = spread(block, "row", NEAR).reshape(count, 3 * columns)
    send = lax.ppermute(attend(True, qkv, out_weight), "col", CORES)
    pair = added(attend(False, qkv, out_weight), send)
    terms = spread(pair, "col", CHIPS)
    half = jnp.sum(terms.astype(jnp.float32), axis=0).astype(jnp.bfloat16)
    rest = lax.ppermute(half, "col", CORES)
    core = lax.rem(lax.axis_index("col"), 2)
    return jnp.concatenate(
        [jnp.where(core == 0, half, rest), jnp.where(core == 0, rest, half)], axis=0
    )


def solution(mesh):
    in_specs = (P("dp", "row"), P("row"), P("row", None, "col"), P("col", "row"))
    out_specs = P("dp", "row")
    return jax.shard_map(shards, mesh=mesh, in_specs=in_specs, out_specs=out_specs, check_vma=False)
```

```python
import math

import jax
import jax.numpy as jnp
from jax import lax
from jax.experimental import pallas as pl
from jax.experimental.pallas import tpu as pltpu
from jax.sharding import PartitionSpec as P

K = 128
EPSILON = 1e-05
LANES = 128
HALF = 64
GROUP = 8
FIELDS = 5
TAIL = 16
LIMIT = pltpu.CompilerParams(vmem_limit_bytes=20 * 2**20)

CLASSES = 4
PLACES = ((1, 3, 4, 6), (0, 2, 5, 7))
NEAR = [[8 * y + place[i] for y in range(2) for place in PLACES] for i in range(4)]
FAR = [[8 * y + z for z in place] for y in range(2) for place in PLACES]
CORES = [(c, c ^ 1) for c in range(8)]
CHIPS = [[0, 2, 4, 6], [1, 3, 5, 7]]


def rounded(a):
    return a.astype(jnp.bfloat16).astype(jnp.float32)


def dot32(a, b):
    return jnp.dot(a, b, preferred_element_type=jnp.float32)


def packed(columns):
    middle, total, square = columns
    tokens = middle.shape[0]
    fields = (
        middle, rounded(total), total - rounded(total), rounded(square), square - rounded(square)
    )
    lane = lax.broadcasted_iota(jnp.int32, (GROUP, LANES), 1)
    tile = jnp.zeros((GROUP, LANES), jnp.float32)
    for group in range(tokens // GROUP):
        for at, field in enumerate(fields):
            tile = jnp.where(
                lane == group * FIELDS + at, field[group * GROUP : (group + 1) * GROUP], tile
            )
    return tile


def moved(tile, lanes):
    return tile if lanes % LANES == 0 else pltpu.roll(tile, -lanes % LANES, 1)


def held_in(tile):
    return tile, moved(tile, 1) + moved(tile, 2), moved(tile, 3) + moved(tile, 4)


def fields_of(middle, total, square):
    lane = lax.broadcasted_iota(jnp.int32, (GROUP, LANES), 1)
    field = lax.rem(lane, FIELDS)
    tile = middle
    for at, number in enumerate(
        (rounded(total), total - rounded(total), rounded(square), square - rounded(square))
    ):
        tile = jnp.where(field == at + 1, moved(number, -1 - at), tile)
    return jnp.where(lane < HALF, tile, 0.0)


def lines_of(tile, tokens):
    return jnp.concatenate(
        [
            jnp.broadcast_to(tile[:, group * FIELDS : group * FIELDS + 1], (GROUP, LANES))
            for group in range(tokens // GROUP)
        ],
        axis=0,
    )


def tail_of(tile, sums):
    row = lax.broadcasted_iota(jnp.int32, (GROUP, LANES), 0)
    lane = lax.broadcasted_iota(jnp.int32, (GROUP, LANES), 1)
    first = jnp.zeros((GROUP, LANES), jnp.float32)
    for at in range(GROUP):
        first = jnp.where(row == at, sums[at], first)
    last = sums[GROUP]
    turned = pltpu.roll(last, HALF, 1)
    second = jnp.where(lane < HALF, tile, jnp.where(row == 0, last, turned))
    return jnp.concatenate([first, second], axis=0)


def sums_of(tail):
    upper = lax.broadcasted_iota(jnp.int32, (1, LANES), 1) >= HALF
    second = tail[GROUP:]
    turned = pltpu.roll(second, HALF, 1)
    return [tail[at : at + 1] for at in range(GROUP)] + [
        jnp.where(upper, second[0:1], turned[1:2])
    ]


def center_kernel(x_ref, o_ref, s_ref):
    count, width = x_ref.shape
    values = x_ref[...].astype(jnp.float32)
    middle = rounded(jnp.sum(values, axis=1, keepdims=True) / width)
    centered = values - middle
    total = jnp.sum(centered, axis=1, keepdims=True)
    square = jnp.sum(centered * centered, axis=1, keepdims=True)
    o_ref[...] = centered
    size = count // CLASSES
    for block in range(CLASSES):
        lines = slice(block * size, (block + 1) * size)
        s_ref[block] = packed((middle[lines], total[lines], square[lines]))


def partial_kernel(x_ref, s_ref, g_ref, w_ref, o_ref):
    tokens, width = x_ref.shape
    size = tokens // CLASSES
    columns = w_ref.shape[2]
    gain = g_ref[...].reshape(1, width)
    high = rounded(gain)
    line = lax.broadcasted_iota(jnp.int32, (16, width), 0)
    gains = jnp.where(line == 0, high, jnp.where(line == 1, gain - high, 0.0)).astype(jnp.bfloat16)
    scaled = jnp.concatenate([(x_ref[...] * gain).astype(jnp.bfloat16), gains], axis=0)
    sums = []
    for part in range(3):
        both = dot32(scaled, w_ref[part])
        product = both[:tokens].astype(jnp.bfloat16)
        c = jnp.sum(both[tokens:], axis=0, keepdims=True)
        for at in range(0, columns, LANES):
            to = len(sums) * size
            for block in range(CLASSES):
                o_ref[block, to : to + size, :] = product[
                    block * size : (block + 1) * size, at : at + LANES
                ]
            sums.append(c[:, at : at + LANES])
    for block in range(CLASSES):
        o_ref[block, len(sums) * size :, :] = tail_of(s_ref[block], sums).astype(jnp.bfloat16)


def merge_kernel(width, r_ref, o_ref):
    blocks = r_ref.shape[0]
    members, rows, _ = o_ref.shape
    chunks = GROUP + 1
    per = (rows - TAIL) // chunks
    size = per * members
    tails = [r_ref[d, chunks * size :, :].astype(jnp.float32) for d in range(blocks)]
    held = [held_in(t[GROUP:]) for t in tails]
    middle = rounded(sum(m + t / width for m, t, _ in held) / blocks)
    shifts = [m - middle for m, _, _ in held]
    total = sum(t + width * s for s, (_, t, _) in zip(shifts, held))
    square = sum(q + 2.0 * s * t + width * (s * s) for s, (_, t, q) in zip(shifts, held))
    sums = [sums_of(t) for t in tails]
    wide = [lines_of(s, size) for s in shifts]
    for at in range(chunks):
        running = jnp.zeros((size, LANES), jnp.float32)
        for d in range(blocks):
            term = r_ref[d, at * size : (at + 1) * size, :].astype(jnp.float32)
            running = running + term + wide[d] * sums[d][at]
        result = running.astype(jnp.bfloat16)
        for member in range(members):
            o_ref[member, at * per : (at + 1) * per, :] = result[member * per : (member + 1) * per]
    merged = [sum(s[at] for s in sums) for at in range(chunks)]
    tile = fields_of(middle, total, square)
    for member in range(members):
        part = moved(tile, member * (per // GROUP) * FIELDS)
        o_ref[member, chunks * per :, :] = tail_of(part, merged).astype(jnp.bfloat16)


def norm_kernel(width, r_ref, o_ref):
    blocks = r_ref.shape[0]
    per, columns = o_ref.shape
    chunks = columns // LANES
    tails = [r_ref[d, chunks * per :, :].astype(jnp.float32) for d in range(blocks)]
    held = [held_in(t[GROUP:]) for t in tails]
    average = sum(m + t / width for m, t, _ in held) / blocks
    shifts = [m - average for m, _, _ in held]
    variance = sum(
        q + 2.0 * s * t + width * (s * s) for s, (_, t, q) in zip(shifts, held)
    ) / (width * blocks)
    scale = lines_of(lax.rsqrt(variance + EPSILON), per)
    wide = [lines_of(s, per) for s in shifts]
    sums = [sums_of(t) for t in tails]
    for at in range(chunks):
        running = jnp.zeros((per, LANES), jnp.float32)
        for d in range(blocks):
            term = r_ref[d, at * per : (at + 1) * per, :].astype(jnp.float32)
            running = running + term + wide[d] * sums[d][at]
        o_ref[:, at * LANES : (at + 1) * LANES] = (running * scale).astype(jnp.bfloat16)


def attend_kernel(other, x_ref, w_ref, o_ref):
    columns = w_ref.shape[0]
    half = o_ref.shape[0]
    core = lax.rem(lax.axis_index("col"), 2)
    which = 1 - core if other else core
    lines = pl.ds(pl.multiple_of(which * half, half), half)
    scaling = 1.0 / math.sqrt(K)
    starts = range(0, columns, K)
    scores = jnp.concatenate(
        [
            lax.dot_general(
                x_ref[lines, at : at + K],
                x_ref[:, columns + at : columns + at + K],
                (((1,), (1,)), ((), ())),
                preferred_element_type=jnp.float32,
            )
            for at in starts
        ],
        axis=0,
    )
    largest = jnp.max(scores, axis=1, keepdims=True)
    exponent = jnp.exp((scores - largest) * scaling)
    inverse = 1.0 / jnp.sum(exponent, axis=1, keepdims=True)
    shares = (exponent * inverse).astype(jnp.bfloat16)
    outs = [
        dot32(
            shares[head * half : (head + 1) * half],
            x_ref[:, 2 * columns + at : 2 * columns + at + K],
        ).astype(jnp.bfloat16)
        for head, at in enumerate(starts)
    ]
    o_ref[...] = dot32(jnp.concatenate(outs, axis=1), w_ref[...]).astype(jnp.bfloat16)


def attend(other, qkv, weight):
    count, wide = qkv.shape
    width = weight.shape[1]
    flops = 2 * (count // 2) * (2 * count * weight.shape[0] + weight.shape[0] * width)
    return pl.pallas_call(
        lambda *refs: attend_kernel(other, *refs),
        out_shape=like((count // 2, width)),
        name="attend",
        compiler_params=LIMIT,
        cost_estimate=pl.CostEstimate(
            flops=4 * flops, bytes_accessed=2 * count * wide, transcendentals=0
        ),
    )(qkv, weight)


def added(a, b):
    return (a.astype(jnp.float32) + b.astype(jnp.float32)).astype(jnp.bfloat16)


def exchange(a, axis, groups):
    return lax.all_to_all(a, axis, 0, 0, tiled=True, axis_index_groups=groups)


def spread(a, axis, groups):
    return exchange(jnp.broadcast_to(a[None], (len(groups[0]), *a.shape)), axis, groups)


def like(shape):
    return jax.ShapeDtypeStruct(shape, jnp.bfloat16)


def shards(tokens, norm_gain, qkv_weight, out_weight):
    count, width = tokens.shape
    columns = qkv_weight.shape[2]
    size = count // CLASSES
    per = size // len(FAR[0])
    chunks = GROUP + 1
    centered, kept = pl.pallas_call(
        center_kernel,
        out_shape=[
            jax.ShapeDtypeStruct((count, width), jnp.float32),
            jax.ShapeDtypeStruct((CLASSES, GROUP, LANES), jnp.float32),
        ],
        name="center",
        compiler_params=LIMIT,
        cost_estimate=pl.CostEstimate(
            flops=2 * 10**9, bytes_accessed=4 * count * width, transcendentals=0
        ),
    )(tokens)
    payload = pl.pallas_call(
        partial_kernel,
        out_shape=like((CLASSES, chunks * size + TAIL, LANES)),
        name="partial",
        compiler_params=LIMIT,
    )(centered, kept, norm_gain, jnp.transpose(qkv_weight, (1, 0, 2)))
    near = exchange(payload, "row", NEAR)
    merged = pl.pallas_call(
        lambda *refs: merge_kernel(width, *refs),
        out_shape=like((len(FAR[0]), chunks * per + TAIL, LANES)),
        name="merge",
        compiler_params=LIMIT,
    )(near)
    far = exchange(merged, "row", FAR)
    mine = pl.pallas_call(
        lambda *refs: norm_kernel(width * CLASSES, *refs),
        out_shape=like((per, 3 * columns)),
        name="norm",
        compiler_params=LIMIT,
    )(far)
    block = spread(mine, "row", FAR).reshape(size, 3 * columns)
    qkv = spread(block, "row", NEAR).reshape(count, 3 * columns)
    send = lax.ppermute(attend(True, qkv, out_weight), "col", CORES)
    pair = added(attend(False, qkv, out_weight), send)
    terms = spread(pair, "col", CHIPS)
    half = jnp.sum(terms.astype(jnp.float32), axis=0).astype(jnp.bfloat16)
    rest = lax.ppermute(half, "col", CORES)
    core = lax.rem(lax.axis_index("col"), 2)
    return jnp.concatenate(
        [jnp.where(core == 0, half, rest), jnp.where(core == 0, rest, half)], axis=0
    )


def solution(mesh):
    in_specs = (P("dp", "row"), P("row"), P("row", None, "col"), P("col", "row"))
    out_specs = P("dp", "row")
    return jax.shard_map(shards, mesh=mesh, in_specs=in_specs, out_specs=out_specs, check_vma=False)
```

```python
import math

import jax
import jax.numpy as jnp
from jax import lax
from jax.experimental import pallas as pl
from jax.experimental.pallas import tpu as pltpu
from jax.sharding import PartitionSpec as P

K = 128
EPSILON = 1e-05
LANES = 128
HALF = 64
GROUP = 8
FIELDS = 5
TAIL = 16
LIMIT = pltpu.CompilerParams(vmem_limit_bytes=20 * 2**20)

CLASSES = 4
PLACES = ((1, 3, 4, 6), (0, 2, 5, 7))
NEAR = [[8 * y + place[i] for y in range(2) for place in PLACES] for i in range(4)]
FAR = [[8 * y + z for z in place] for y in range(2) for place in PLACES]
CORES = [(c, c ^ 1) for c in range(8)]
CHIPS = [[0, 2, 4, 6], [1, 3, 5, 7]]


def rounded(a):
    return a.astype(jnp.bfloat16).astype(jnp.float32)


def dot32(a, b):
    return jnp.dot(a, b, preferred_element_type=jnp.float32)


def packed(columns):
    middle, total, square = columns
    tokens = middle.shape[0]
    fields = (
        middle, rounded(total), total - rounded(total), rounded(square), square - rounded(square)
    )
    lane = lax.broadcasted_iota(jnp.int32, (GROUP, LANES), 1)
    tile = jnp.zeros((GROUP, LANES), jnp.float32)
    for group in range(tokens // GROUP):
        for at, field in enumerate(fields):
            tile = jnp.where(
                lane == group * FIELDS + at, field[group * GROUP : (group + 1) * GROUP], tile
            )
    return tile


def moved(tile, lanes):
    return tile if lanes % LANES == 0 else pltpu.roll(tile, -lanes % LANES, 1)


def held_in(tile):
    return tile, moved(tile, 1) + moved(tile, 2), moved(tile, 3) + moved(tile, 4)


def fields_of(middle, total, square):
    lane = lax.broadcasted_iota(jnp.int32, (GROUP, LANES), 1)
    field = lax.rem(lane, FIELDS)
    tile = middle
    for at, number in enumerate(
        (rounded(total), total - rounded(total), rounded(square), square - rounded(square))
    ):
        tile = jnp.where(field == at + 1, moved(number, -1 - at), tile)
    return jnp.where(lane < HALF, tile, 0.0)


def lines_of(tile, tokens):
    return jnp.concatenate(
        [
            jnp.broadcast_to(tile[:, group * FIELDS : group * FIELDS + 1], (GROUP, LANES))
            for group in range(tokens // GROUP)
        ],
        axis=0,
    )


def tail_of(tile, sums):
    row = lax.broadcasted_iota(jnp.int32, (GROUP, LANES), 0)
    lane = lax.broadcasted_iota(jnp.int32, (GROUP, LANES), 1)
    first = jnp.zeros((GROUP, LANES), jnp.float32)
    for at in range(GROUP):
        first = jnp.where(row == at, sums[at], first)
    last = sums[GROUP]
    turned = pltpu.roll(last, HALF, 1)
    second = jnp.where(lane < HALF, tile, jnp.where(row == 0, last, turned))
    return jnp.concatenate([first, second], axis=0)


def sums_of(tail):
    upper = lax.broadcasted_iota(jnp.int32, (1, LANES), 1) >= HALF
    second = tail[GROUP:]
    turned = pltpu.roll(second, HALF, 1)
    return [tail[at : at + 1] for at in range(GROUP)] + [
        jnp.where(upper, second[0:1], turned[1:2])
    ]


def center_kernel(x_ref, o_ref, s_ref):
    count, width = x_ref.shape
    values = x_ref[...].astype(jnp.float32)
    middle = rounded(jnp.sum(values, axis=1, keepdims=True) / width)
    centered = values - middle
    total = jnp.sum(centered, axis=1, keepdims=True)
    square = jnp.sum(centered * centered, axis=1, keepdims=True)
    o_ref[...] = centered
    size = count // CLASSES
    for block in range(CLASSES):
        lines = slice(block * size, (block + 1) * size)
        s_ref[block] = packed((middle[lines], total[lines], square[lines]))


def partial_kernel(x_ref, s_ref, g_ref, w_ref, o_ref):
    tokens, width = x_ref.shape
    size = tokens // CLASSES
    columns = w_ref.shape[2]
    gain = g_ref[...].reshape(1, width)
    high = rounded(gain)
    line = lax.broadcasted_iota(jnp.int32, (16, width), 0)
    gains = jnp.where(line == 0, high, jnp.where(line == 1, gain - high, 0.0)).astype(jnp.bfloat16)
    scaled = jnp.concatenate([(x_ref[...] * gain).astype(jnp.bfloat16), gains], axis=0)
    sums = []
    for part in range(3):
        both = dot32(scaled, w_ref[part])
        product = both[:tokens].astype(jnp.bfloat16)
        c = jnp.sum(both[tokens:], axis=0, keepdims=True)
        for at in range(0, columns, LANES):
            to = len(sums) * size
            for block in range(CLASSES):
                o_ref[block, to : to + size, :] = product[
                    block * size : (block + 1) * size, at : at + LANES
                ]
            sums.append(c[:, at : at + LANES])
    for block in range(CLASSES):
        o_ref[block, len(sums) * size :, :] = tail_of(s_ref[block], sums).astype(jnp.bfloat16)


def merge_kernel(width, r_ref, o_ref):
    blocks = r_ref.shape[0]
    members, rows, _ = o_ref.shape
    chunks = GROUP + 1
    per = (rows - TAIL) // chunks
    size = per * members
    tails = [r_ref[d, chunks * size :, :].astype(jnp.float32) for d in range(blocks)]
    held = [held_in(t[GROUP:]) for t in tails]
    middle = rounded(sum(m + t / width for m, t, _ in held) / blocks)
    shifts = [m - middle for m, _, _ in held]
    total = sum(t + width * s for s, (_, t, _) in zip(shifts, held))
    square = sum(q + 2.0 * s * t + width * (s * s) for s, (_, t, q) in zip(shifts, held))
    sums = [sums_of(t) for t in tails]
    wide = [lines_of(s, size) for s in shifts]
    for at in range(chunks):
        running = jnp.zeros((size, LANES), jnp.float32)
        for d in range(blocks):
            term = r_ref[d, at * size : (at + 1) * size, :].astype(jnp.float32)
            running = running + term + wide[d] * sums[d][at]
        result = running.astype(jnp.bfloat16)
        for member in range(members):
            o_ref[member, at * per : (at + 1) * per, :] = result[member * per : (member + 1) * per]
    merged = [sum(s[at] for s in sums) for at in range(chunks)]
    tile = fields_of(middle, total, square)
    for member in range(members):
        part = moved(tile, member * (per // GROUP) * FIELDS)
        o_ref[member, chunks * per :, :] = tail_of(part, merged).astype(jnp.bfloat16)


def norm_kernel(width, r_ref, o_ref):
    blocks = r_ref.shape[0]
    per, columns = o_ref.shape
    chunks = columns // LANES
    tails = [r_ref[d, chunks * per :, :].astype(jnp.float32) for d in range(blocks)]
    held = [held_in(t[GROUP:]) for t in tails]
    average = sum(m + t / width for m, t, _ in held) / blocks
    shifts = [m - average for m, _, _ in held]
    variance = sum(
        q + 2.0 * s * t + width * (s * s) for s, (_, t, q) in zip(shifts, held)
    ) / (width * blocks)
    scale = lines_of(lax.rsqrt(variance + EPSILON), per)
    wide = [lines_of(s, per) for s in shifts]
    sums = [sums_of(t) for t in tails]
    for at in range(chunks):
        running = jnp.zeros((per, LANES), jnp.float32)
        for d in range(blocks):
            term = r_ref[d, at * per : (at + 1) * per, :].astype(jnp.float32)
            running = running + term + wide[d] * sums[d][at]
        o_ref[:, at * LANES : (at + 1) * LANES] = (running * scale).astype(jnp.bfloat16)


def attend_kernel(other, x_ref, w_ref, o_ref):
    columns = w_ref.shape[0]
    half = o_ref.shape[0]
    core = lax.rem(lax.axis_index("col"), 2)
    which = 1 - core if other else core
    lines = pl.ds(pl.multiple_of(which * half, half), half)
    scaling = 1.0 / math.sqrt(K)
    starts = range(0, columns, K)
    scores = jnp.concatenate(
        [
            lax.dot_general(
                x_ref[lines, at : at + K],
                x_ref[:, columns + at : columns + at + K],
                (((1,), (1,)), ((), ())),
                preferred_element_type=jnp.float32,
            )
            for at in starts
        ],
        axis=0,
    )
    largest = jnp.max(scores, axis=1, keepdims=True)
    exponent = jnp.exp((scores - largest) * scaling)
    inverse = 1.0 / jnp.sum(exponent, axis=1, keepdims=True)
    shares = exponent.astype(jnp.bfloat16)
    outs = [
        (
            dot32(
                shares[head * half : (head + 1) * half],
                x_ref[:, 2 * columns + at : 2 * columns + at + K],
            )
            * inverse[head * half : (head + 1) * half]
        ).astype(jnp.bfloat16)
        for head, at in enumerate(starts)
    ]
    o_ref[...] = dot32(jnp.concatenate(outs, axis=1), w_ref[...]).astype(jnp.bfloat16)


def attend(other, qkv, weight):
    count, wide = qkv.shape
    width = weight.shape[1]
    flops = 2 * (count // 2) * (2 * count * weight.shape[0] + weight.shape[0] * width)
    return pl.pallas_call(
        lambda *refs: attend_kernel(other, *refs),
        out_shape=like((count // 2, width)),
        name="attend",
        compiler_params=LIMIT,
        cost_estimate=pl.CostEstimate(
            flops=4 * flops, bytes_accessed=2 * count * wide, transcendentals=0
        ),
    )(qkv, weight)


def write_kernel(own_ref, rest_ref, o_ref, sems):
    half = own_ref.shape[0]
    core = lax.rem(lax.axis_index("col"), 2)
    copies = [
        pltpu.make_async_copy(
            ref, o_ref.at[pl.ds(pl.multiple_of(at * half, half), half), :], sems.at[slot]
        )
        for slot, (ref, at) in enumerate(((own_ref, core), (rest_ref, 1 - core)))
    ]
    for copy in copies:
        copy.start()
    for copy in copies:
        copy.wait()


def added(a, b):
    return (a.astype(jnp.float32) + b.astype(jnp.float32)).astype(jnp.bfloat16)


def exchange(a, axis, groups):
    return lax.all_to_all(a, axis, 0, 0, tiled=True, axis_index_groups=groups)


def spread(a, axis, groups):
    return exchange(jnp.broadcast_to(a[None], (len(groups[0]), *a.shape)), axis, groups)


def like(shape):
    return jax.ShapeDtypeStruct(shape, jnp.bfloat16)


def shards(tokens, norm_gain, qkv_weight, out_weight):
    count, width = tokens.shape
    columns = qkv_weight.shape[2]
    size = count // CLASSES
    per = size // len(FAR[0])
    chunks = GROUP + 1
    centered, kept = pl.pallas_call(
        center_kernel,
        out_shape=[
            jax.ShapeDtypeStruct((count, width), jnp.float32),
            jax.ShapeDtypeStruct((CLASSES, GROUP, LANES), jnp.float32),
        ],
        name="center",
        compiler_params=LIMIT,
        cost_estimate=pl.CostEstimate(
            flops=2 * 10**9, bytes_accessed=4 * count * width, transcendentals=0
        ),
    )(tokens)
    payload = pl.pallas_call(
        partial_kernel,
        out_shape=like((CLASSES, chunks * size + TAIL, LANES)),
        name="partial",
        compiler_params=LIMIT,
    )(centered, kept, norm_gain, jnp.transpose(qkv_weight, (1, 0, 2)))
    near = exchange(payload, "row", NEAR)
    merged = pl.pallas_call(
        lambda *refs: merge_kernel(width, *refs),
        out_shape=like((len(FAR[0]), chunks * per + TAIL, LANES)),
        name="merge",
        compiler_params=LIMIT,
    )(near)
    far = exchange(merged, "row", FAR)
    mine = pl.pallas_call(
        lambda *refs: norm_kernel(width * CLASSES, *refs),
        out_shape=like((per, 3 * columns)),
        name="norm",
        compiler_params=LIMIT,
    )(far)
    block = spread(mine, "row", FAR).reshape(size, 3 * columns)
    qkv = spread(block, "row", NEAR).reshape(count, 3 * columns)
    send = lax.ppermute(attend(True, qkv, out_weight), "col", CORES)
    pair = added(attend(False, qkv, out_weight), send)
    terms = spread(pair, "col", CHIPS)
    half = jnp.sum(terms.astype(jnp.float32), axis=0).astype(jnp.bfloat16)
    rest = lax.ppermute(half, "col", CORES)
    return pl.pallas_call(
        write_kernel,
        out_shape=like((count, width)),
        out_specs=pl.BlockSpec(memory_space=pl.ANY),
        scratch_shapes=[pltpu.SemaphoreType.DMA((2,))],
        name="write",
        compiler_params=LIMIT,
    )(half, rest)


def solution(mesh):
    in_specs = (P("dp", "row"), P("row"), P("row", None, "col"), P("col", "row"))
    out_specs = P("dp", "row")
    return jax.shard_map(shards, mesh=mesh, in_specs=in_specs, out_specs=out_specs, check_vma=False)
```
